256 devices in a mesh: lat: 16 (over z, core), lon: 8 (over x, y_hi), ens: 2 (over y_lo).
Axes of the slice: x: 4, y: 4 (y_hi: 2, y_lo: 2; y = y_hi * 2 + y_lo), z: 8, core: 2. Of those that a mesh axis runs over, the one named last changes fastest.
Arguments:
- state: bfloat16 [4, 96, 192, 768], P('ens', 'lat', 'lon'), parts along dimension 0, may hold values from -6 to 6
- spec_weight1: float32 [2, 8, 96, 96], P(None, 'lon'), may hold values from -0.4375 to 0.4375
- spec_bias1: float32 [2, 8, 96], P(None, 'lon'), may hold values from -0.6 to 0.6
- spec_weight2: float32 [2, 8, 96, 96], P(None, 'lon'), may hold values from -0.4375 to 0.4375
- spec_bias2: float32 [2, 8, 96], P(None, 'lon'), may hold values from -0.12 to 0.12
- norm1_gain: float32 [768], replicated, may hold values from 0.5 to 1.5
- norm1_bias: float32 [768], replicated, may hold values from -0.6 to 0.6
- norm2_gain: float32 [768], replicated, may hold values from 0.5 to 1.5
- norm2_bias: float32 [768], replicated, may hold values from -0.6 to 0.6
- fc1_weight: bfloat16 [768, 3072], replicated, may hold values from -0.21875 to 0.21875
- fc1_bias: float32 [3072], replicated, may hold values from -0.6 to 0.6
- fc2_weight: bfloat16 [3072, 768], replicated, may hold values from -0.109375 to 0.109375
- fc2_bias: float32 [768], replicated, may hold values from -0.6 to 0.6
- cotangent: bfloat16 [4, 96, 192, 768], P('ens', 'lat', 'lon'), parts along dimension 0, may hold values from -6 to 6
Outputs:
- advanced: bfloat16 [4, 96, 192, 768], P('ens', 'lat', 'lon'), parts along dimension 0
- sensitivity: bfloat16 [4, 96, 192, 768], P('ens', 'lat', 'lon'), parts along dimension 0
The draws below stay inside these ranges and needn't reach their ends.
There are 2 independent parts, one for each index of `ens`. The reference program is written for one: setup_inputs(seed, part) draws one part's arguments, and reference() takes and returns one part's arrays. A program takes and returns all parts, laid end to end along the dimension named above; an argument that names none is the same for every part. Nothing has to cross between parts.
All inputs are finite; a program needn't handle non-finite values.
Results may differ from the reference program's by a relative error of at most 0.0085.
Values may be sent and summed in bfloat16 or wider, within the bound.
A program may use at most 128 MiB of HBM per device.

```python
import jax
import jax.numpy as jnp
from jax import lax

D = 768
FF = 3072
NB = 8
BS = 96
B = 2
H = 96
W = 192


def steps_of(stream_key, extent, cuts, least, largest):
    loudness, own = 1.0, jax.random.fold_in(stream_key, 6)
    for position, shards_of in cuts:
        steps = jnp.exp(jax.random.uniform(jax.random.fold_in(own, position), (shards_of,), jnp.float32, least / len(cuts), largest / len(cuts)))
        loudness = loudness * jnp.repeat(steps, extent[position] // shards_of).reshape([-1 if axis == position else 1 for axis in range(len(extent))])
    return loudness


def scatter_about(own_key, extent, spread, limit, shards=(), kind=jnp.bfloat16):
    drawn = jax.random.normal(own_key, extent, jnp.float32) * spread
    if len(shards) > 0:
        drawn = steps_of(own_key, extent, shards, -0.22, 0.18) * drawn
    return jnp.clip(drawn, min=-limit, max=limit).astype(kind)


def setup_inputs(seed: int = 0, part: int = 0) -> dict:
    streams_of = jax.random.split(jax.random.key(seed), 15)
    part_splits = jax.random.split(jax.random.fold_in(streams_of[14], part), 15)
    return {
        "state": scatter_about(part_splits[0], (B, H, W, D), 1.0, 6.0, ((1, 16), (2, 8))),
        "spec_weight1": scatter_about(streams_of[1], (2, NB, BS, BS), (2 * BS) ** -0.5, 0.4375, ((1, 8),), jnp.float32),
        "spec_bias1": scatter_about(streams_of[2], (2, NB, BS), 0.1, 0.6, ((1, 8),), jnp.float32),
        "spec_weight2": scatter_about(streams_of[3], (2, NB, BS, BS), (2 * BS) ** -0.5, 0.4375, ((1, 8),), jnp.float32),
        "spec_bias2": scatter_about(streams_of[4], (2, NB, BS), 0.02, 0.12, ((1, 8),), jnp.float32),
        "norm1_gain": jnp.clip(1.0 + 0.1 * jax.random.normal(streams_of[5], (D,), jnp.float32), 0.5, 1.5),
        "norm1_bias": scatter_about(streams_of[6], (D,), 0.1, 0.6, (), jnp.float32),
        "norm2_gain": jnp.clip(1.0 + 0.1 * jax.random.normal(streams_of[7], (D,), jnp.float32), 0.5, 1.5),
        "norm2_bias": scatter_about(streams_of[8], (D,), 0.1, 0.6, (), jnp.float32),
        "fc1_weight": scatter_about(streams_of[9], (D, FF), D ** -0.5, 0.21875),
        "fc1_bias": scatter_about(streams_of[10], (FF,), 0.1, 0.6, (), jnp.float32),
        "fc2_weight": scatter_about(streams_of[11], (FF, D), FF ** -0.5, 0.109375),
        "fc2_bias": scatter_about(streams_of[12], (D,), 0.1, 0.6, (), jnp.float32),
        "cotangent": scatter_about(part_splits[13], (B, H, W, D), 1.0, 6.0, ((1, 16), (2, 8))),
    }


HIGH = lax.Precision.HIGHEST
EPSILON = 1e-06
THRESHOLD = 0.01

def layer_norm(values, gain, shift):
    average = lax.optimization_barrier(jnp.mean(values, axis=-1, keepdims=True))
    centred = values - average
    inverse = lax.rsqrt(lax.optimization_barrier(jnp.mean(centred * centred, axis=-1, keepdims=True)) + EPSILON)
    normed = centred * inverse
    return (normed * gain + shift, normed, inverse)

def norm_backward(gradient, gain, normed, inverse):
    scaled = gradient * gain
    return inverse * (scaled - lax.optimization_barrier(jnp.mean(scaled, axis=-1, keepdims=True)) - normed * lax.optimization_barrier(jnp.mean(scaled * normed, axis=-1, keepdims=True)))

def gelu_exact(values):
    return jax.nn.gelu(values, approximate=False)

def gelu_slope(values):
    cumulative = 0.5 * (1.0 + lax.erf(values * 0.7071067811865476))
    density = jnp.exp(-0.5 * values * values) * 0.3989422804014327
    return cumulative + values * density

def block_product(real_part, imag_part, weight):
    blocks, width = (weight.shape[1], weight.shape[2])
    shape = real_part.shape
    real_split = real_part.reshape(shape[:-1] + (blocks, width))
    imag_split = imag_part.reshape(shape[:-1] + (blocks, width))

    def multiply(values, matrix):
        return jnp.einsum('...nb,nbo->...no', values, matrix, precision=HIGH).reshape(shape)
    return (multiply(real_split, weight[0]) - multiply(imag_split, weight[1]), multiply(real_split, weight[1]) + multiply(imag_split, weight[0]))

def block_adjoint(real_part, imag_part, weight):
    blocks, width = (weight.shape[1], weight.shape[2])
    shape = real_part.shape
    real_split = real_part.reshape(shape[:-1] + (blocks, width))
    imag_split = imag_part.reshape(shape[:-1] + (blocks, width))

    def multiply(values, matrix):
        return jnp.einsum('...no,nbo->...nb', values, matrix, precision=HIGH).reshape(shape)
    return (multiply(real_split, weight[0]) + multiply(imag_split, weight[1]), multiply(imag_split, weight[0]) - multiply(real_split, weight[1]))

def forward_transform(field):
    spectrum = jnp.fft.fft2(field, axes=(1, 2), norm='ortho')
    return (jnp.real(spectrum), jnp.imag(spectrum))

def inverse_real(real_part, imag_part):
    return jnp.real(jnp.fft.ifft2(lax.complex(real_part, imag_part), axes=(1, 2), norm='ortho'))

def reference(state, spec_weight1, spec_bias1, spec_weight2, spec_bias2, norm1_gain, norm1_bias, norm2_gain, norm2_bias, fc1_weight, fc1_bias, fc2_weight, fc2_bias, cotangent):
    source = state.astype(jnp.float32)
    normed_one, hat_one, inverse_one = layer_norm(source, norm1_gain, norm1_bias)
    lowered = normed_one.astype(jnp.bfloat16)
    spec_real, spec_imag = forward_transform(lowered.astype(jnp.float32))
    first_real, first_imag = block_product(spec_real, spec_imag, spec_weight1)
    first_real = first_real + spec_bias1[0].reshape(-1)
    first_imag = first_imag + spec_bias1[1].reshape(-1)
    second_real, second_imag = block_product(gelu_exact(first_real), gelu_exact(first_imag), spec_weight2)
    second_real = second_real + spec_bias2[0].reshape(-1)
    second_imag = second_imag + spec_bias2[1].reshape(-1)
    shrunk_real = second_real - THRESHOLD * jnp.tanh(second_real / THRESHOLD)
    shrunk_imag = second_imag - THRESHOLD * jnp.tanh(second_imag / THRESHOLD)
    filtered = inverse_real(shrunk_real, shrunk_imag)
    mixed = (filtered + lowered.astype(jnp.float32) + source).astype(jnp.bfloat16)

    def token_rows(row_pair):
        mixed_rows, cot_rows = row_pair
        mixed_float = mixed_rows.astype(jnp.float32)
        normed_two, hat_two, inverse_two = layer_norm(mixed_float, norm2_gain, norm2_bias)
        hidden_pre = jnp.dot(normed_two.astype(jnp.bfloat16), fc1_weight, preferred_element_type=jnp.float32) + fc1_bias
        hidden = gelu_exact(hidden_pre).astype(jnp.bfloat16)
        advanced_rows = (jnp.dot(hidden, fc2_weight, preferred_element_type=jnp.float32) + fc2_bias + mixed_float).astype(jnp.bfloat16)
        grad_hidden = jnp.dot(cot_rows, fc2_weight.T, preferred_element_type=jnp.float32)
        grad_pre = (grad_hidden * gelu_slope(hidden_pre)).astype(jnp.bfloat16)
        grad_normed = jnp.dot(grad_pre, fc1_weight.T, preferred_element_type=jnp.float32)
        grad_rows = (cot_rows.astype(jnp.float32) + norm_backward(grad_normed, norm2_gain, hat_two, inverse_two)).astype(jnp.bfloat16)
        return (advanced_rows, grad_rows)
    row_shape = (-1,) + mixed.shape[2:]
    advanced, grad_mixed = lax.map(token_rows, (mixed.reshape(row_shape), cotangent.reshape(row_shape)))
    advanced = advanced.reshape(state.shape)
    grad_mixed = grad_mixed.reshape(state.shape)
    grad_float = grad_mixed.astype(jnp.float32)
    gs_real, gs_imag = forward_transform(grad_float)
    slope_real = jnp.tanh(second_real / THRESHOLD)
    slope_imag = jnp.tanh(second_imag / THRESHOLD)
    gq_real = gs_real * slope_real * slope_real
    gq_imag = gs_imag * slope_imag * slope_imag
    ga_real, ga_imag = block_adjoint(gq_real, gq_imag, spec_weight2)
    gp_real = ga_real * gelu_slope(first_real)
    gp_imag = ga_imag * gelu_slope(first_imag)
    gz_real, gz_imag = block_adjoint(gp_real, gp_imag, spec_weight1)
    grad_lowered = inverse_real(gz_real, gz_imag) + grad_float
    sensitivity = (grad_float + norm_backward(grad_lowered, norm1_gain, hat_one, inverse_one)).astype(jnp.bfloat16)
    return (advanced, sensitivity)
```

```python
import math

import jax
import jax.numpy as jnp
import numpy as np
from jax import lax
from jax.experimental import pallas as pl
from jax.experimental.pallas import tpu as pltpu
from jax.sharding import PartitionSpec as P

EPSILON = 1e-06
THRESHOLD = 0.01
F32 = jnp.float32
BF16 = jnp.bfloat16

NP = 16
NJ = 8
R = 6
C = 24
TOK = R * C
KS = 6
H = NP * R
W = NJ * C
BS = 96
D = 768
FF = 3072
HC = 512
ROWS = 2 * KS * H

roll = pltpu.roll


def tables():
    def cs(rows, cols, modulus):
        angle = 2.0 * np.pi * (np.outer(rows, cols) % modulus) / modulus
        return np.cos(angle) / math.sqrt(modulus), np.sin(angle) / math.sqrt(modulus)

    w = np.arange(W)
    cosine, sine = cs(w, np.arange(W // 2), W)
    parity = (1.0 - 2.0 * (w % 2)) / math.sqrt(W)
    ahead = np.zeros((NP, 16, W))
    even = np.zeros((W, NP, 16))
    odd = np.zeros((W, NP, 16))
    for p in range(NP):
        for kc in range(12):
            c, k = divmod(kc, KS)
            f = p * KS + k
            if c == 0:
                row, back = cosine[:, f], (2.0 if f else 1.0) * cosine[:, f]
            else:
                row, back = (-sine[:, f], -2.0 * sine[:, f]) if f else (parity, parity)
            ahead[p, kc] = row
            if kc < 8:
                even[:, p, kc] = back
                odd[:, p, kc] = back
            else:
                ahead[p, kc + 4] = row
                even[:, p, kc] = back
                odd[:, p, kc + 4] = back
    ahead = ahead.reshape(NP * 16, W)
    even = even.reshape(W, NP * 16)
    odd = odd.reshape(W, NP * 16)
    g = np.arange(H)
    co, si = cs(g, g, H)
    zero = np.zeros_like(co)
    fwd = np.block([[co, si], [-si, co]])
    inv = np.block([[co, -si], [si, co]])
    fwd0 = np.stack(
        [
            np.block([[co, si], [-si, co], [co, si], [si, -co]]),
            np.block([[co, zero], [-si, zero], [zero, co], [zero, -si]]),
        ]
    )
    inv0 = np.stack(
        [
            0.5 * np.block([[co, -si, co, si], [si, co, si, -co]]),
            np.block([[co, -si, zero, zero], [zero, zero, co, -si]]),
        ]
    )
    return [ahead, even, odd, fwd, 0.5 * inv, fwd0, inv0]


def split_table(table):
    high = np.asarray(table, np.float32).astype(jnp.bfloat16)
    low = (np.asarray(table, np.float64) - high.astype(np.float64)).astype(np.float32).astype(jnp.bfloat16)
    return np.stack([high, low])


def dot(a, b):
    return jnp.dot(a, b, preferred_element_type=F32)


def dot_nt(a, b):
    return lax.dot_general(a, b, (((1,), (1,)), ((), ())), preferred_element_type=F32)


def table_dot(high, low, x):
    x = x.astype(BF16)
    return dot(high, x) + dot(low, x)


def lanes():
    return lax.broadcasted_iota(jnp.int32, (1, 128), 1)


def layer_norm(values):
    average = jnp.mean(values, axis=-1, keepdims=True)
    centred = values - average
    inverse = lax.rsqrt(jnp.mean(centred * centred, axis=-1, keepdims=True) + EPSILON)
    return centred * inverse, inverse


def norm_backward(gradient, gain, normed, inverse):
    scaled = gradient * gain
    return inverse * (
        scaled
        - jnp.mean(scaled, axis=-1, keepdims=True)
        - normed * jnp.mean(scaled * normed, axis=-1, keepdims=True)
    )


def cumulative(values):
    return 0.5 * (1.0 + lax.erf(values * 0.7071067811865476))


def density(values):
    return jnp.exp(-0.5 * values * values) * 0.3989422804014327


def feature_block(tile, b):
    t, o = divmod(BS * b, 128)
    if o == 0:
        return tile(t)
    first = roll(tile(t), 128 - o, 1)
    if o == 32:
        return first
    return jnp.where(lanes() < 128 - o, first, roll(tile(t + 1), 128 - o, 1))


def joined_blocks(blocks):
    lane = lanes()
    tiles = []
    for q in (0, 4):
        one, two, three = roll(blocks[q + 1], 96, 1), roll(blocks[q + 2], 64, 1), roll(blocks[q + 3], 32, 1)
        tiles += [
            jnp.where(lane < 96, blocks[q], one),
            jnp.where(lane < 64, one, two),
            jnp.where(lane < 32, two, three),
        ]
    return jnp.concatenate(tiles, axis=1)


def pack_lon(m):
    lane = lanes()
    extra = m[112:144]
    parts = [jnp.where(lane < 96, m[32 * i : 32 * i + 32], roll(extra, 96 - 32 * i, 1) if i < 3 else extra) for i in range(3)]
    return jnp.concatenate(parts + [m[96:112]], axis=0)


def unpack_lon(m):
    lane = lanes()
    extra = jnp.where(
        lane < 32, roll(m[0:32], 32, 1), jnp.where(lane < 64, roll(m[32:64], 64, 1), roll(m[64:96], 96, 1))
    )
    return jnp.concatenate([m, extra], axis=0)


def pack_lat(t):
    lane = lanes()
    out = []
    for i in range(R):
        shift = 96 - 32 * (i % 3)
        out.append(jnp.where(lane < 96, t[i], roll(t[7 + i // 3], shift, 1)))
    return jnp.concatenate(out + [t[6]], axis=0)


def unpack_lat(m):
    lane = lanes()
    t = [m[8 * i : 8 * i + 8] for i in range(7)]
    for e in range(2):
        a, b, c = t[3 * e : 3 * e + 3]
        t.append(jnp.where(lane < 32, roll(a, 32, 1), jnp.where(lane < 64, roll(b, 64, 1), roll(c, 96, 1))))
    return t


def unpack_rows(recv, wide, peers=range(NJ)):
    for j in peers:
        m = unpack_lon(recv(j).astype(F32))
        for r in range(R):
            wide[C * j : C * j + C, 128 * r : 128 * r + 128] = m[C * r : C * r + C]


def width_ahead(recv, wide, tall, ahead, put):
    unpack_rows(recv, wide)
    tall[...] = table_dot(ahead[0], ahead[1], wide[...])
    upper = lax.broadcasted_iota(jnp.int32, (8, 1), 0) < 4
    for p in range(NP):
        def rows(r, at):
            return tall[16 * p + at : 16 * p + at + 8, 128 * r : 128 * r + 128]
        t = [rows(r, 0) for r in range(R)]
        t += [jnp.where(upper, rows(2 * i, 8), rows(2 * i + 1, 8)) for i in range(3)]
        put(p, pack_lat(t))


def slot_rows(kc, eights, fours):
    if kc < 8:
        return eights, pl.ds(kc, H, stride=8)
    return fours, pl.ds(kc - 8, H, stride=4)


def height_ahead(recv, eights, fours, wide, spec, fwd, fwd0):
    for p in range(NP):
        t = unpack_lat(recv(p).astype(F32))
        eights[48 * p : 48 * p + 48, :] = jnp.concatenate(t[:6], axis=0)
        fours[24 * p : 24 * p + 24, :] = jnp.concatenate(t[6:], axis=0)
    for c in range(2):
        for k in range(KS):
            ref, rows = slot_rows(c * KS + k, eights, fours)
            wide[H * c : H * c + H, 128 * k : 128 * k + 128] = ref[rows, :]
    zero = table_dot(fwd0[0], fwd0[1], wide[:, 0:128])
    rest = table_dot(fwd[0], fwd[1], wide[:, 128:])
    half = KS * H
    spec[0:H, 0:128] = zero[0:H]
    spec[0:H, 128:256] = zero[H : 2 * H]
    spec[half : half + H, 0:128] = zero[2 * H : 3 * H]
    spec[half : half + H, 128:256] = zero[3 * H :]
    for k in range(1, KS):
        real, imag = rest[0:H, 128 * (k - 1) : 128 * k], rest[H:, 128 * (k - 1) : 128 * k]
        spec[H * k : H * k + H, 0:128] = real
        spec[H * k : H * k + H, 128:256] = imag
        spec[half + H * k : half + H * k + H, 0:128] = real
        spec[half + H * k : half + H * k + H, 128:256] = -imag


def height_back(spec, eights, fours, wide, first, inv, inv0, put):
    half = KS * H
    for i, (at, lane) in enumerate(((0, 0), (0, 128), (half, 0), (half, 128))):
        first[H * i : H * i + H, :] = spec[at : at + H, lane : lane + 128]
    for k in range(1, KS):
        low = spec[H * k : H * k + H, :]
        high = spec[half + H * k : half + H * k + H, :]
        wide[0:H, 128 * k : 128 * k + 128] = low[:, 0:128] + high[:, 0:128]
        wide[H : 2 * H, 128 * k : 128 * k + 128] = low[:, 128:] - high[:, 128:]
    zero = table_dot(inv0[0], inv0[1], first[...])
    rest = table_dot(inv[0], inv[1], wide[:, 128:])
    for c in range(2):
        for k in range(KS):
            ref, rows = slot_rows(c * KS + k, eights, fours)
            values = zero[H * c : H * c + H] if k == 0 else rest[H * c : H * c + H, 128 * (k - 1) : 128 * k]
            ref[rows, :] = values
    for p in range(NP):
        t = [eights[48 * p + 8 * i : 48 * p + 8 * i + 8, :] for i in range(6)]
        t += [fours[24 * p + 8 * i : 24 * p + 8 * i + 8, :] for i in range(3)]
        put(p, pack_lat(t))


def width_back(recv, tall, even, odd, put):
    for p in range(NP):
        t = unpack_lat(recv(p).astype(F32))
        for r in range(R):
            at = 128 * (r // 2) + 384 * (r % 2)
            tall[16 * p : 16 * p + 8, at : at + 128] = t[r]
            tall[16 * p + 8 : 16 * p + 16, at : at + 128] = t[6 + r // 2]
    fields = (table_dot(even[0], even[1], tall[:, 0:384]), table_dot(odd[0], odd[1], tall[:, 384:768]))
    for j in range(NJ):
        m = [fields[r % 2][C * j : C * j + C, 128 * (r // 2) : 128 * (r // 2) + 128] for r in range(R)]
        put(j, pack_lon(jnp.concatenate(m, axis=0)))


def gathered(recv):
    return joined_blocks([unpack_lon(recv(b).astype(F32))[:, 0:128] for b in range(NJ)])


def matrix_dot(values, matrix):
    return dot(values.astype(BF16), matrix[0])


def matrix_dot_nt(values, matrix):
    return dot_nt(values.astype(BF16), matrix[0])


CHUNK = 192


def spectral_ahead(loop, spec, first_pre, squares, mat1, bias1, mat2, bias2):
    def step(i):
        rows = pl.ds(pl.multiple_of(i * CHUNK, CHUNK), CHUNK)
        pre = matrix_dot(spec[rows, :], mat1) + bias1[...]
        first_pre[rows, :] = pre
        second = matrix_dot(pre * cumulative(pre), mat2) + bias2[...]
        slope = jnp.tanh(second * (1.0 / THRESHOLD))
        squares[rows, :] = slope * slope
        spec[rows, :] = second - THRESHOLD * slope
    loop(ROWS // CHUNK, step)


def spectral_slopes(loop, first_pre):
    def step(i):
        rows = pl.ds(pl.multiple_of(i * CHUNK, CHUNK), CHUNK)
        pre = first_pre[rows, :]
        first_pre[rows, :] = cumulative(pre) + pre * density(pre)
    loop(ROWS // CHUNK, step)


def spectral_adjoint(loop, spec, slopes, squares, mat1, mat2):
    def step(i):
        rows = pl.ds(pl.multiple_of(i * CHUNK, CHUNK), CHUNK)
        grad = matrix_dot_nt(spec[rows, :] * squares[rows, :], mat2)
        spec[rows, :] = matrix_dot_nt(grad * slopes[rows, :], mat1)
    loop(ROWS // CHUNK, step)


def fill_matrix(out, weight):
    out[...] = jnp.zeros_like(out)
    real, imag = weight[0, 0], weight[1, 0]
    out[0, 0:BS, 0:BS] = real.astype(BF16)
    out[0, 0:BS, 128 : 128 + BS] = imag.astype(BF16)
    out[0, 128 : 128 + BS, 0:BS] = (-imag).astype(BF16)
    out[0, 128 : 128 + BS, 128 : 128 + BS] = real.astype(BF16)


def fill_bias(out, bias):
    out[...] = jnp.zeros_like(out)
    out[0:1, 0:BS] = bias[0]
    out[0:1, 128 : 128 + BS] = bias[1]


def token_ahead(loop, mixed, cot, held, fc1, bias1, gain2, shift2, hidden, gh, acc):
    normed, inverse = layer_norm(mixed)
    v = (normed * gain2 + shift2).astype(BF16)
    acc[...] = jnp.zeros_like(acc)

    def step(n):
        cols = pl.ds(pl.multiple_of(n * HC, HC), HC)
        pre = dot(v, fc1[:, cols]) + bias1[:, cols]
        phi = cumulative(pre)
        hidden[held, cols] = (pre * phi).astype(BF16)
        grad = (gh[held, cols] * (phi + pre * density(pre))).astype(BF16)
        acc[...] += dot_nt(grad, fc1[:, cols])
    loop(FF // HC, step)
    return (cot + norm_backward(acc[...], gain2, normed, inverse)).astype(BF16).astype(F32)


def kernel(
    state, weight1, bias_1, weight2, bias_2, gain1, shift1, gain2, shift2, fc1_hbm, fc1_bias, fc2_hbm, fc2_bias, cotangent,
    ahead, even, odd, fwd, inv, fwd0_both, inv0_both,
    advanced, sensitivity,
    fc1, fc2, lon_send, lon_recv, lat_send, lat_recv, lowered, mixed, grads, hidden, gh, acc,
    wide, tall, eights, fours, first, spec, first_pre, squares, mat1, mat2, bias1, bias2, fwd0, inv0,
    load_sem, lon_send_sem, lon_recv_sem, lat_send_sem, lat_recv_sem,
):
    p = lax.axis_index("lat")
    j = lax.axis_index("lon")

    def loop(count, body):
        lax.fori_loop(0, count, lambda i, _: (body(i), 0)[1], 0)

    barrier = pltpu.get_barrier_semaphore()
    for d in range(1, NP):
        pl.semaphore_signal(barrier, inc=1, device_id={"lat": lax.rem(p + d, NP)}, device_id_type=pl.DeviceIdType.MESH)
    for d in range(1, NJ):
        pl.semaphore_signal(barrier, inc=1, device_id={"lon": lax.rem(j + d, NJ)}, device_id_type=pl.DeviceIdType.MESH)
    load2 = pltpu.make_async_copy(fc2_hbm, fc2, load_sem.at[0])
    load1 = pltpu.make_async_copy(fc1_hbm, fc1, load_sem.at[1])
    load2.start()
    load1.start()

    def sending(x, s, axis):
        e = 2 * x + s
        if axis == "lon":
            return lon_send, lon_recv, lon_send_sem, lon_recv_sem, e, NJ, j
        return lat_send, lat_recv, lat_send_sem, lat_recv_sem, e, NP, p

    def putter(x, s, axis):
        send, recv, _, _, e, n, me = sending(x, s, axis)

        def put(to, values):
            send[e, to] = values.astype(BF16)
        return put

    def copy(x, s, axis, to):
        send, recv, send_sem, recv_sem, e, n, me = sending(x, s, axis)
        return pltpu.make_async_remote_copy(
            src_ref=send.at[e, to],
            dst_ref=recv.at[e, me],
            send_sem=send_sem.at[e],
            recv_sem=recv_sem.at[e],
            device_id={axis: to},
            device_id_type=pl.DeviceIdType.MESH,
        )

    def go(x, s, axis):
        send, recv, _, _, e, n, me = sending(x, s, axis)
        for i in range(1, n):
            d = n - i // 2 if i % 2 else i // 2
            d = (i + 1) // 2 if i % 2 else n - i // 2
            copy(x, s, axis, lax.rem(me + d, n)).start()
        recv[e, me] = send[e, me]

    def all_but_one(x, s, axis):
        send, recv, send_sem, recv_sem, e, n, me = sending(x, s, axis)
        return pltpu.make_async_remote_copy(
            src_ref=send.at[e, pl.ds(0, n - 1)],
            dst_ref=recv.at[e, pl.ds(0, n - 1)],
            send_sem=send_sem.at[e],
            recv_sem=recv_sem.at[e],
            device_id={axis: lax.rem(me + 1, n)},
            device_id_type=pl.DeviceIdType.MESH,
        )

    def arrived(x, s, axis):
        all_but_one(x, s, axis).wait_recv()
        _, recv, _, _, e, _, _ = sending(x, s, axis)
        return lambda k: recv[e, k]

    def tokens(ref, s):
        return jnp.concatenate([ref[s, r].astype(F32) for r in range(R)], axis=0)

    def out_tokens(ref, s, values):
        for r in range(R):
            ref[s, r] = values[C * r : C * r + C].astype(BF16)

    def held(s):
        return pl.ds(TOK * s, TOK)

    def send_tokens(x, s, ref):
        put = putter(x, s, "lon")
        for b in range(NJ):
            put(b, pack_lon(feature_block(lambda t: ref[s, :, 128 * t : 128 * t + 128], b)))

    for s in range(2):
        normed, _ = layer_norm(tokens(state, s))
        lowered[s] = (normed * gain1[...] + shift1[...]).astype(BF16).astype(F32)
        send_tokens(0, s, lowered)
        if s == 0:
            pl.semaphore_wait(barrier, NP + NJ - 2)
        go(0, s, "lon")
    fill_matrix(mat1, weight1)
    fill_matrix(mat2, weight2)
    fill_bias(bias1, bias_1)
    fill_bias(bias2, bias_2)
    packed = p == 0
    fwd0[...] = jnp.where(packed, fwd0_both[1], fwd0_both[0])
    inv0[...] = jnp.where(packed, inv0_both[1], inv0_both[0])

    for s in range(2):
        width_ahead(arrived(0, s, "lon"), wide, tall, ahead, putter(0, s, "lat"))
        go(0, s, "lat")

    load2.wait()
    cots = jnp.concatenate([tokens(cotangent, s) for s in range(2)], axis=0).astype(BF16)

    def cot_step(n):
        cols = pl.ds(pl.multiple_of(n * HC, HC), HC)
        gh[:, cols] = dot_nt(cots, fc2[cols, :])
    loop(FF // HC, cot_step)

    for s in range(2):
        height_ahead(arrived(0, s, "lat"), eights, fours, wide, spec, fwd, fwd0)
        spectral_ahead(loop, spec, first_pre.at[s], squares.at[s], mat1, bias1, mat2, bias2)
        height_back(spec, eights, fours, wide, first, inv, inv0, putter(1, s, "lat"))
        go(1, s, "lat")
    for s in range(2):
        spectral_slopes(loop, first_pre.at[s])
    load1.wait()
    for s in range(2):
        width_back(arrived(1, s, "lat"), tall, even, odd, putter(1, s, "lon"))
        go(1, s, "lon")
    for s in range(2):
        filtered = gathered(arrived(1, s, "lon"))
        mixed[s] = (filtered + lowered[s] + tokens(state, s)).astype(BF16).astype(F32)
        grads[s] = token_ahead(
            loop, mixed[s], tokens(cotangent, s), held(s), fc1, fc1_bias, gain2[...], shift2[...], hidden, gh, acc
        )
        send_tokens(2, s, grads)
        go(2, s, "lon")

    def advance(s):
        for n in range(D // 256):
            cols = slice(256 * n, 256 * n + 256)
            values = dot(hidden[TOK * s : TOK * s + TOK, :], fc2[:, cols]) + fc2_bias[:, cols] + mixed[s, :, cols]
            for r in range(R):
                advanced[s, r, :, cols] = values[C * r : C * r + C].astype(BF16)

    for s in range(2):
        width_ahead(arrived(2, s, "lon"), wide, tall, ahead, putter(2, s, "lat"))
        go(2, s, "lat")
    for s in range(2):
        advance(s)
    for s in range(2):
        height_ahead(arrived(2, s, "lat"), eights, fours, wide, spec, fwd, fwd0)
        spectral_adjoint(loop, spec, first_pre.at[s], squares.at[s], mat1, mat2)
        height_back(spec, eights, fours, wide, first, inv, inv0, putter(3, s, "lat"))
        go(3, s, "lat")
    for s in range(2):
        width_back(arrived(3, s, "lat"), tall, even, odd, putter(3, s, "lon"))
        go(3, s, "lon")
    for s in range(2):
        grad = grads[s]
        grad_lowered = gathered(arrived(3, s, "lon")) + grad
        normed, inverse = layer_norm(tokens(state, s))
        out_tokens(sensitivity, s, grad + norm_backward(grad_lowered, gain1[...], normed, inverse))
    for x in range(4):
        for s in range(2):
            all_but_one(x, s, "lon").wait_send()
            all_but_one(x, s, "lat").wait_send()


def shards(
    state, spec_weight1, spec_bias1, spec_weight2, spec_bias2, norm1_gain, norm1_bias, norm2_gain, norm2_bias,
    fc1_weight, fc1_bias, fc2_weight, fc2_bias, cotangent,
):
    vmem = pl.BlockSpec(memory_space=pltpu.VMEM)
    hbm = pl.BlockSpec(memory_space=pl.ANY)
    names = [jnp.asarray(split_table(t)) if t.ndim == 2 else jnp.asarray(np.stack([split_table(x) for x in t])) for t in tables()]
    row = lambda a: a.reshape(1, -1)
    operands = [
        state, spec_weight1, spec_bias1, spec_weight2, spec_bias2, row(norm1_gain), row(norm1_bias), row(norm2_gain),
        row(norm2_bias), fc1_weight, row(fc1_bias), fc2_weight, row(fc2_bias), cotangent, *names,
    ]
    specs = [hbm if i in (9, 11) else vmem for i in range(len(operands))]
    out = jax.ShapeDtypeStruct(state.shape, BF16)
    return pl.pallas_call(
        kernel,
        out_shape=(out, out),
        in_specs=specs,
        out_specs=(vmem, vmem),
        scratch_shapes=[
            pltpu.VMEM((D, FF), BF16),
            pltpu.VMEM((FF, D), BF16),
            pltpu.VMEM((8, NJ, 112, 128), BF16),
            pltpu.VMEM((8, NJ, 112, 128), BF16),
            pltpu.VMEM((8, NP, 56, 128), BF16),
            pltpu.VMEM((8, NP, 56, 128), BF16),
            pltpu.VMEM((2, TOK, D), F32),
            pltpu.VMEM((2, TOK, D), F32),
            pltpu.VMEM((2, TOK, D), F32),
            pltpu.VMEM((2 * TOK, FF), BF16),
            pltpu.VMEM((2 * TOK, FF), F32),
            pltpu.VMEM((TOK, D), F32),
            pltpu.VMEM((W, D), F32),
            pltpu.VMEM((16 * NP, D), F32),
            pltpu.VMEM((8 * H, 128), F32),
            pltpu.VMEM((4 * H, 128), F32),
            pltpu.VMEM((4 * H, 128), F32),
            pltpu.VMEM((ROWS, 256), F32),
            pltpu.VMEM((2, ROWS, 256), F32),
            pltpu.VMEM((2, ROWS, 256), F32),
            pltpu.VMEM((1, 256, 256), BF16),
            pltpu.VMEM((1, 256, 256), BF16),
            pltpu.VMEM((1, 256), F32),
            pltpu.VMEM((1, 256), F32),
            pltpu.VMEM((2, 4 * H, 2 * H), BF16),
            pltpu.VMEM((2, 2 * H, 4 * H), BF16),
            pltpu.SemaphoreType.DMA((2,)),
            pltpu.SemaphoreType.DMA((8,)),
            pltpu.SemaphoreType.DMA((8,)),
            pltpu.SemaphoreType.DMA((8,)),
            pltpu.SemaphoreType.DMA((8,)),
        ],
        compiler_params=pltpu.CompilerParams(
            collective_id=0, has_side_effects=True, vmem_limit_bytes=60 * 1024 * 1024
        ),
        name="block",
    )(*operands)


def solution(mesh):
    in_specs = (
        P("ens", "lat", "lon", None),
        P(None, "lon", None, None),
        P(None, "lon", None),
        P(None, "lon", None, None),
        P(None, "lon", None),
        P(), P(), P(), P(), P(), P(), P(), P(),
        P("ens", "lat", "lon", None),
    )
    out_specs = (P("ens", "lat", "lon", None), P("ens", "lat", "lon", None))
    return jax.shard_map(shards, mesh=mesh, in_specs=in_specs, out_specs=out_specs, check_vma=False)
```

```python
import math

import jax
import jax.numpy as jnp
import numpy as np
from jax import lax
from jax.experimental import pallas as pl
from jax.experimental.pallas import tpu as pltpu
from jax.sharding import PartitionSpec as P

EPSILON = 1e-06
THRESHOLD = 0.01
F32 = jnp.float32
BF16 = jnp.bfloat16

NP = 16
NJ = 8
R = 6
C = 24
TOK = R * C
KS = 6
H = NP * R
W = NJ * C
BS = 96
D = 768
FF = 3072
HC = 512
ROWS = 2 * KS * H
FIRST, MIDDLE, LAST = [0, 5, 6], [1, 2, 3, 4, 7, 8, 10, 12, 13, 14, 15, 16, 17, 18], [11, 9]

roll = pltpu.roll


def tables():
    def cs(rows, cols, modulus):
        angle = 2.0 * np.pi * (np.outer(rows, cols) % modulus) / modulus
        return np.cos(angle) / math.sqrt(modulus), np.sin(angle) / math.sqrt(modulus)

    w = np.arange(W)
    cosine, sine = cs(w, np.arange(W // 2), W)
    parity = (1.0 - 2.0 * (w % 2)) / math.sqrt(W)
    ahead = np.zeros((NP, 16, W))
    even = np.zeros((W, NP, 16))
    odd = np.zeros((W, NP, 16))
    for p in range(NP):
        for kc in range(12):
            c, k = divmod(kc, KS)
            f = p * KS + k
            if c == 0:
                row, back = cosine[:, f], (2.0 if f else 1.0) * cosine[:, f]
            else:
                row, back = (-sine[:, f], -2.0 * sine[:, f]) if f else (parity, parity)
            ahead[p, kc] = row
            if kc < 8:
                even[:, p, kc] = back
                odd[:, p, kc] = back
            else:
                ahead[p, kc + 4] = row
                even[:, p, kc] = back
                odd[:, p, kc + 4] = back
    ahead = ahead.reshape(NP * 16, W)
    even = even.reshape(W, NP * 16)
    odd = odd.reshape(W, NP * 16)
    g = np.arange(H)
    co, si = cs(g, g, H)
    fwd = np.block([[co, si], [-si, co]])
    inv = 0.5 * np.block([[co, -si], [si, co]])
    return [split_table(ahead), split_table(fwd), rounded(even), rounded(odd), rounded(inv)]


def rounded(table):
    return np.asarray(table, np.float32).astype(jnp.bfloat16)


def split_table(table):
    high = np.asarray(table, np.float32).astype(jnp.bfloat16)
    low = (np.asarray(table, np.float64) - high.astype(np.float64)).astype(np.float32).astype(jnp.bfloat16)
    return np.stack([high, low])


def dot(a, b):
    return jnp.dot(a, b, preferred_element_type=F32)


def dot_nt(a, b):
    return lax.dot_general(a, b, (((1,), (1,)), ((), ())), preferred_element_type=F32)


def table_dot(table, x):
    x = x.astype(BF16)
    if len(table.shape) == 2:
        return dot(table[...], x)
    return dot(table[0], x) + dot(table[1], x)


def row(ref):
    return ref[...].reshape(1, -1)


def lanes():
    return lax.broadcasted_iota(jnp.int32, (1, 128), 1)


def layer_norm(values):
    average = jnp.mean(values, axis=-1, keepdims=True)
    centred = values - average
    inverse = lax.rsqrt(jnp.mean(centred * centred, axis=-1, keepdims=True) + EPSILON)
    return centred * inverse, inverse


def norm_backward(gradient, gain, normed, inverse):
    scaled = gradient * gain
    return inverse * (
        scaled
        - jnp.mean(scaled, axis=-1, keepdims=True)
        - normed * jnp.mean(scaled * normed, axis=-1, keepdims=True)
    )


def cumulative(values):
    return 0.5 * (1.0 + lax.erf(values * 0.7071067811865476))


def density(values):
    return jnp.exp(-0.5 * values * values) * 0.3989422804014327


def feature_block(tile, b):
    t, o = divmod(BS * b, 128)
    if o == 0:
        return tile(t)
    first = roll(tile(t), 128 - o, 1)
    if o == 32:
        return first
    return jnp.where(lanes() < 128 - o, first, roll(tile(t + 1), 128 - o, 1))


def joined_blocks(blocks):
    lane = lanes()
    tiles = []
    for q in (0, 4):
        one, two, three = roll(blocks[q + 1], 96, 1), roll(blocks[q + 2], 64, 1), roll(blocks[q + 3], 32, 1)
        tiles += [
            jnp.where(lane < 96, blocks[q], one),
            jnp.where(lane < 64, one, two),
            jnp.where(lane < 32, two, three),
        ]
    return jnp.concatenate(tiles, axis=1)


def pack_lon(m):
    lane = lanes()
    extra = m[112:144]
    parts = [jnp.where(lane < 96, m[32 * i : 32 * i + 32], roll(extra, 96 - 32 * i, 1) if i < 3 else extra) for i in range(3)]
    return jnp.concatenate(parts + [m[96:112]], axis=0)


def unpack_lon(m):
    lane = lanes()
    extra = jnp.where(
        lane < 32, roll(m[0:32], 32, 1), jnp.where(lane < 64, roll(m[32:64], 64, 1), roll(m[64:96], 96, 1))
    )
    return jnp.concatenate([m, extra], axis=0)


def pack_lat(t):
    lane = lanes()
    out = []
    for i in range(R):
        shift = 96 - 32 * (i % 3)
        out.append(jnp.where(lane < 96, t[i], roll(t[7 + i // 3], shift, 1)))
    return jnp.concatenate(out + [t[6]], axis=0)


def unpack_lat(m):
    lane = lanes()
    t = [m[8 * i : 8 * i + 8] for i in range(7)]
    for e in range(2):
        a, b, c = t[3 * e : 3 * e + 3]
        t.append(jnp.where(lane < 32, roll(a, 32, 1), jnp.where(lane < 64, roll(b, 64, 1), roll(c, 96, 1))))
    return t


def at(index, size, count=None, offset=0):
    return pl.ds(pl.multiple_of(index * size + offset, 8), count or size)


def width_ahead(froms, recv, wide, tall, ahead, tos, put):
    for group in froms:
        recv.wait(group)
        for j in group:
            m = unpack_lon(recv(j).astype(F32))
            for r in range(R):
                wide[at(j, C), 128 * r : 128 * r + 128] = m[C * r : C * r + C]
    tall[...] = table_dot(ahead, wide[...])
    upper = lax.broadcasted_iota(jnp.int32, (8, 1), 0) < 4
    for group in tos:
        for p in group:
            def rows(r, offset):
                return tall[at(p, 16, 8, offset), 128 * r : 128 * r + 128]
            t = [rows(r, 0) for r in range(R)]
            t += [jnp.where(upper, rows(2 * i, 8), rows(2 * i + 1, 8)) for i in range(3)]
            put(p, pack_lat(t))
        put.send(group)


def slot_rows(kc, eights, fours):
    if kc < 8:
        return eights, pl.ds(kc, H, stride=8)
    return fours, pl.ds(kc - 8, H, stride=4)


def height_ahead(froms, recv, eights, fours, wide, spec, fwd, fwd0):
    for group in froms:
        recv.wait(group)
        for p in group:
            t = unpack_lat(recv(p).astype(F32))
            eights[at(p, 48), :] = jnp.concatenate(t[:6], axis=0)
            fours[at(p, 24), :] = jnp.concatenate(t[6:], axis=0)
    for c in range(2):
        for k in range(KS):
            ref, rows = slot_rows(c * KS + k, eights, fours)
            wide[H * c : H * c + H, 128 * k : 128 * k + 128] = ref[rows, :]
    zero = table_dot(fwd0, wide[:, 0:128])
    rest = table_dot(fwd, wide[:, 128:])
    half = KS * H
    spec[0:H, 0:128] = zero[0:H]
    spec[0:H, 128:256] = zero[H : 2 * H]
    spec[half : half + H, 0:128] = zero[2 * H : 3 * H]
    spec[half : half + H, 128:256] = zero[3 * H :]
    for k in range(1, KS):
        real, imag = rest[0:H, 128 * (k - 1) : 128 * k], rest[H:, 128 * (k - 1) : 128 * k]
        spec[H * k : H * k + H, 0:128] = real
        spec[H * k : H * k + H, 128:256] = imag
        spec[half + H * k : half + H * k + H, 0:128] = real
        spec[half + H * k : half + H * k + H, 128:256] = -imag


def height_back(spec, eights, fours, wide, first, inv, inv0, tos, put):
    half = KS * H
    for i, (start, lane) in enumerate(((0, 0), (0, 128), (half, 0), (half, 128))):
        first[H * i : H * i + H, :] = spec[start : start + H, lane : lane + 128]
    for k in range(1, KS):
        low = spec[H * k : H * k + H, :]
        high = spec[half + H * k : half + H * k + H, :]
        wide[0:H, 128 * k : 128 * k + 128] = low[:, 0:128] + high[:, 0:128]
        wide[H : 2 * H, 128 * k : 128 * k + 128] = low[:, 128:] - high[:, 128:]
    zero = table_dot(inv0, first[...])
    rest = table_dot(inv, wide[:, 128:])
    for c in range(2):
        for k in range(KS):
            ref, rows = slot_rows(c * KS + k, eights, fours)
            values = zero[H * c : H * c + H] if k == 0 else rest[H * c : H * c + H, 128 * (k - 1) : 128 * k]
            ref[rows, :] = values
    for group in tos:
        for p in group:
            t = [eights[at(p, 48, 8, 8 * i), :] for i in range(6)]
            t += [fours[at(p, 24, 8, 8 * i), :] for i in range(3)]
            put(p, pack_lat(t))
        put.send(group)


def width_back(froms, recv, tall, wide, even, odd, tos, put):
    for group in froms:
        recv.wait(group)
        for p in group:
            t = unpack_lat(recv(p).astype(F32))
            for r in range(R):
                lane = 128 * (r // 2) + 384 * (r % 2)
                tall[at(p, 16, 8), lane : lane + 128] = t[r]
                tall[at(p, 16, 8, 8), lane : lane + 128] = t[6 + r // 2]
    wide[:, 0:384] = table_dot(even, tall[:, 0:384])
    wide[:, 384:768] = table_dot(odd, tall[:, 384:768])
    for group in tos:
        for j in group:
            m = [wide[at(j, C), 128 * (r // 2) + 384 * (r % 2) : 128 * (r // 2) + 384 * (r % 2) + 128] for r in range(R)]
            put(j, pack_lon(jnp.concatenate(m, axis=0)))
        put.send(group)


def gathered(recv):
    recv.wait(range(NJ))
    return joined_blocks([unpack_lon(recv(b).astype(F32))[:, 0:128] for b in range(NJ)])


def matrix_dot(values, matrix):
    return dot(values.astype(BF16), matrix[0])


def matrix_dot_nt(values, matrix):
    return dot_nt(values.astype(BF16), matrix[0])


CHUNK = 192


def spectral_ahead(loop, spec, first_pre, squares, mat1, bias1, mat2, bias2):
    def step(i):
        rows = pl.ds(pl.multiple_of(i * CHUNK, CHUNK), CHUNK)
        pre = matrix_dot(spec[rows, :], mat1) + bias1[...]
        first_pre[rows, :] = pre
        second = matrix_dot(pre * cumulative(pre), mat2) + bias2[...]
        slope = jnp.tanh(second * (1.0 / THRESHOLD))
        squares[rows, :] = slope * slope
        spec[rows, :] = second - THRESHOLD * slope
    loop(ROWS // CHUNK, step)


def spectral_slopes(loop, first_pre):
    def step(i):
        rows = pl.ds(pl.multiple_of(i * CHUNK, CHUNK), CHUNK)
        pre = first_pre[rows, :]
        first_pre[rows, :] = cumulative(pre) + pre * density(pre)
    loop(ROWS // CHUNK, step)


def spectral_adjoint(loop, spec, slopes, squares, mat1, mat2):
    def step(i):
        rows = pl.ds(pl.multiple_of(i * CHUNK, CHUNK), CHUNK)
        grad = matrix_dot_nt(spec[rows, :] * squares[rows, :], mat2)
        spec[rows, :] = matrix_dot_nt(grad * slopes[rows, :], mat1)
    loop(ROWS // CHUNK, step)


def fill_matrix(out, weight):
    out[...] = jnp.zeros_like(out)
    real, imag = weight[0, 0], weight[1, 0]
    out[0, 0:BS, 0:BS] = real.astype(BF16)
    out[0, 0:BS, 128 : 128 + BS] = imag.astype(BF16)
    out[0, 128 : 128 + BS, 0:BS] = (-imag).astype(BF16)
    out[0, 128 : 128 + BS, 128 : 128 + BS] = real.astype(BF16)


def fill_first(fwd0, inv0, fwd, inv, packed):
    left = lax.broadcasted_iota(jnp.int32, (1, 2 * H), 1) < H
    one = jnp.where(packed, 0.0, 1.0)
    first = jnp.where(left, 1.0, one)
    second = jnp.where(left, one, 1.0)
    for i in range(2):
        real, imag = fwd[i, 0:H].astype(F32), fwd[i, H : 2 * H].astype(F32)
        fwd0[i, 0:H] = (real * first).astype(BF16)
        fwd0[i, H : 2 * H] = (imag * first).astype(BF16)
        fwd0[i, 2 * H : 3 * H] = (jnp.where(packed, imag, real) * second).astype(BF16)
        fwd0[i, 3 * H : 4 * H] = (-jnp.where(packed, real, imag) * second).astype(BF16)
    real, imag = inv[0:H].astype(F32), inv[H : 2 * H].astype(F32)
    sign = jnp.where(left, 1.0, -1.0)
    inv0[0:H, 0 : 2 * H] = jnp.where(packed, 2.0 * real, real).astype(BF16)
    inv0[H : 2 * H, 0 : 2 * H] = (imag * one).astype(BF16)
    inv0[0:H, 2 * H : 4 * H] = (real * sign * one).astype(BF16)
    inv0[H : 2 * H, 2 * H : 4 * H] = jnp.where(packed, 2.0 * real, imag * sign).astype(BF16)


def fill_bias(out, bias):
    out[...] = jnp.zeros_like(out)
    out[0:1, 0:BS] = bias[0]
    out[0:1, 128 : 128 + BS] = bias[1]


def token_ahead(loop, mixed, cot, held, fc1, bias1, gain2, shift2, hidden, gh, acc):
    normed, inverse = layer_norm(mixed)
    v = (normed * gain2 + shift2).astype(BF16)
    acc[...] = jnp.zeros_like(acc)

    def step(n):
        cols = pl.ds(pl.multiple_of(n * HC, HC), HC)
        pre = dot(v, fc1[:, cols]) + bias1[cols].reshape(1, -1)
        phi = cumulative(pre)
        hidden[held, cols] = (pre * phi).astype(BF16)
        grad = (gh[held, cols] * (phi + pre * density(pre))).astype(BF16)
        acc[...] += dot_nt(grad, fc1[:, cols])
    loop(FF // HC, step)
    return (cot + norm_backward(acc[...], gain2, normed, inverse)).astype(BF16).astype(F32)


def kernel(
    *refs,
):
    sources, rest = refs[:19], refs[19:]
    (
        advanced, sensitivity,
        state, weight1, bias_1, weight2, bias_2, gain1, shift1, gain2, shift2, fc1, fc1_bias, fc2, fc2_bias, cotangent,
        ahead, fwd, even, odd, inv,
        lon_send, lon_recv, lat_send, lat_recv, lowered, mixed, grads, hidden, gh, acc,
        wide, tall, eights, fours, first, spec, first_pre, squares, mat1, mat2, bias1, bias2, fwd0, inv0,
        load_sem, lon_send_sem, lon_recv_sem, lat_send_sem, lat_recv_sem,
    ) = rest
    p = lax.axis_index("lat")
    j = lax.axis_index("lon")

    def loop(count, body):
        lax.fori_loop(0, count, lambda i, _: (body(i), 0)[1], 0)

    ens = lax.axis_index("ens")
    lon_ring = [(dx, dy) for dx in (2, 1, 3, 0) for dy in (0, 1)]
    lat_ring = [(dz, dc) for dz in (4, 3, 5, 2, 6, 1, 7, 0) for dc in (0, 1)]

    def lon_peers(sign):
        return [lax.rem(j // 2 + 4 + sign * dx, 4) * 2 + lax.rem(j + dy, 2) for dx, dy in lon_ring]

    def lat_peers(sign):
        return [lax.rem(p // 2 + 8 + sign * dz, 8) * 2 + lax.rem(p + dc, 2) for dz, dc in lat_ring if dz + dc]

    lon_to, lon_from, lat_to, lat_from = lon_peers(1), lon_peers(-1), lat_peers(1), lat_peers(-1)

    def device(axis, to):
        return {"lon": to, "ens": 1 - ens} if axis == "lon" else {"lat": to}

    barrier = pltpu.get_barrier_semaphore()
    for axis, peers in (("lat", lat_to), ("lon", lon_to)):
        for to in peers:
            pl.semaphore_signal(barrier, inc=1, device_id=device(axis, to), device_id_type=pl.DeviceIdType.MESH)
    held_here = (
        state, weight1, bias_1, weight2, bias_2, gain1, shift1, gain2, shift2, fc1, fc1_bias, fc2, fc2_bias, cotangent,
        ahead, fwd, even, odd, inv,
    )
    loads = [pltpu.make_async_copy(a, b, load_sem.at[i]) for i, (a, b) in enumerate(zip(sources, held_here))]
    for i in FIRST + MIDDLE + LAST:
        loads[i].start()
    for i in FIRST:
        loads[i].wait()

    def buffers(x, s, axis):
        e = 2 * x + s
        if axis == "lon":
            return lon_send, lon_recv, lon_send_sem, lon_recv_sem, e, j
        return lat_send, lat_recv, lat_send_sem, lat_recv_sem, e, p

    def copy(x, s, axis, to, slot):
        send, recv, send_sem, recv_sem, e, me = buffers(x, s, axis)
        return pltpu.make_async_remote_copy(
            src_ref=send.at[e, to],
            dst_ref=recv.at[e, slot],
            send_sem=send_sem.at[e],
            recv_sem=recv_sem.at[e, slot],
            device_id=device(axis, to),
            device_id_type=pl.DeviceIdType.MESH,
        )

    class Sender:
        def __init__(self, x, s, axis):
            self.where = (x, s, axis)

        def __call__(self, to, values):
            send, recv, _, _, e, _ = buffers(*self.where)
            (recv if to is p else send)[e, to] = values.astype(BF16)

        def send(self, group):
            me = buffers(*self.where)[-1]
            for to in group:
                if to is not p:
                    copy(*self.where, to, me).start()

    class Receiver:
        def __init__(self, x, s, axis):
            self.where = (x, s, axis)

        def wait(self, group):
            for source in group:
                if source is not p:
                    copy(*self.where, source, source).wait_recv()

        def __call__(self, source):
            _, recv, _, _, e, _ = buffers(*self.where)
            return recv[e, source]

    sender, receiver = Sender, Receiver

    def halves(peers):
        return [peers[: len(peers) // 2], peers[len(peers) // 2 :]]

    def sent(x, s, axis, count):
        send, recv, send_sem, recv_sem, e, me = buffers(x, s, axis)
        pltpu.make_async_remote_copy(
            src_ref=send.at[e, pl.ds(0, count)],
            dst_ref=recv.at[e, pl.ds(0, count)],
            send_sem=send_sem.at[e],
            recv_sem=recv_sem.at[e, 0],
            device_id=device(axis, lon_to[0] if axis == "lon" else lat_to[0]),
            device_id_type=pl.DeviceIdType.MESH,
        ).wait_send()

    def tokens(ref, s):
        return jnp.concatenate([ref[s, r].astype(F32) for r in range(R)], axis=0)

    def out_tokens(ref, s, values):
        for r in range(R):
            ref[s, r] = values[C * r : C * r + C].astype(BF16)

    def held(s):
        return pl.ds(TOK * s, TOK)

    def send_tokens(x, s, ref):
        e = 2 * x + s
        for b in range(NJ):
            lon_send[e, b] = pack_lon(feature_block(lambda t: ref[s, :, 128 * t : 128 * t + 128], b)).astype(BF16)
        if e == 0:
            pl.semaphore_wait(barrier, NP - 1 + NJ)
        for to in lon_to:
            copy(x, s, "lon", to, j).start()

    for s in range(2):
        with jax.named_scope("ln"):
            normed, _ = layer_norm(tokens(state, s))
            lowered[s] = (normed * row(gain1) + row(shift1)).astype(BF16).astype(F32)
            send_tokens(0, s, lowered)
    for i in MIDDLE:
        loads[i].wait()
    fill_matrix(mat1, weight1)
    fill_matrix(mat2, weight2)
    fill_bias(bias1, bias_1)
    fill_bias(bias2, bias_2)
    fill_first(fwd0, inv0, fwd, inv, p == 0)

    for s in range(2):
        with jax.named_scope("w0"):
            width_ahead(halves(lon_from), receiver(0, s, "lon"), wide, tall, ahead, halves(lat_to + [p]), sender(0, s, "lat"))

    with jax.named_scope("gh"):
        loads[11].wait()
        cots = jnp.concatenate([tokens(cotangent, s) for s in range(2)], axis=0).astype(BF16)

        def cot_step(n):
            cols = pl.ds(pl.multiple_of(n * HC, HC), HC)
            gh[:, cols] = dot_nt(cots, fc2[cols, :])
        loop(FF // HC, cot_step)

    for s in range(2):
        with jax.named_scope("h0"):
            height_ahead(halves([p] + lat_from), receiver(0, s, "lat"), eights, fours, wide, spec, fwd, fwd0)
        with jax.named_scope("sp0"):
            spectral_ahead(loop, spec, first_pre.at[s], squares.at[s], mat1, bias1, mat2, bias2)
        with jax.named_scope("hb1"):
            height_back(spec, eights, fours, wide, first, inv, inv0, halves(lat_to + [p]), sender(1, s, "lat"))
    for s in range(2):
        with jax.named_scope("slopes"):
            spectral_slopes(loop, first_pre.at[s])
    loads[9].wait()
    for s in range(2):
        with jax.named_scope("wb1"):
            width_back(halves([p] + lat_from), receiver(1, s, "lat"), tall, wide, even, odd, halves(lon_to), sender(1, s, "lon"))
    for s in range(2):
        with jax.named_scope("gath1"):
            filtered = gathered(receiver(1, s, "lon"))
            mixed[s] = (filtered + lowered[s] + tokens(state, s)).astype(BF16).astype(F32)
        with jax.named_scope("token"):
            grads[s] = token_ahead(
                loop, mixed[s], tokens(cotangent, s), held(s), fc1, fc1_bias, row(gain2), row(shift2), hidden, gh, acc
            )
        with jax.named_scope("sendt"):
            send_tokens(2, s, grads)

    def advance(s):
        for n in range(D // 256):
            cols = slice(256 * n, 256 * n + 256)
            values = dot(hidden[TOK * s : TOK * s + TOK, :], fc2[:, cols]) + fc2_bias[cols].reshape(1, -1) + mixed[s, :, cols]
            for r in range(R):
                advanced[s, r, :, cols] = values[C * r : C * r + C].astype(BF16)

    for s in range(2):
        with jax.named_scope("w2"):
            width_ahead(halves(lon_from), receiver(2, s, "lon"), wide, tall, ahead, halves(lat_to + [p]), sender(2, s, "lat"))
    for s in range(2):
        with jax.named_scope("adv"):
            advance(s)
    for s in range(2):
        with jax.named_scope("h2"):
            height_ahead(halves([p] + lat_from), receiver(2, s, "lat"), eights, fours, wide, spec, fwd, fwd0)
        with jax.named_scope("sp2"):
            spectral_adjoint(loop, spec, first_pre.at[s], squares.at[s], mat1, mat2)
        with jax.named_scope("hb3"):
            height_back(spec, eights, fours, wide, first, inv, inv0, halves(lat_to + [p]), sender(3, s, "lat"))
    for s in range(2):
        with jax.named_scope("wb3"):
            width_back(halves([p] + lat_from), receiver(3, s, "lat"), tall, wide, even, odd, halves(lon_to), sender(3, s, "lon"))
    for s in range(2):
        with jax.named_scope("final"):
            grad = grads[s]
            grad_lowered = gathered(receiver(3, s, "lon")) + grad
            normed, inverse = layer_norm(tokens(state, s))
            out_tokens(sensitivity, s, grad + norm_backward(grad_lowered, row(gain1), normed, inverse))
    for x in range(4):
        for s in range(2):
            sent(x, s, "lon", NJ)
            sent(x, s, "lat", NP - 1)


def finish(advanced, sensitivity, advanced_out, sensitivity_out):
    advanced_out[...] = advanced[...]
    sensitivity_out[...] = sensitivity[...]


def shards(
    state, spec_weight1, spec_bias1, spec_weight2, spec_bias2, norm1_gain, norm1_bias, norm2_gain, norm2_bias,
    fc1_weight, fc1_bias, fc2_weight, fc2_bias, cotangent,
):
    vmem = pl.BlockSpec(memory_space=pltpu.VMEM)
    hbm = pl.BlockSpec(memory_space=pltpu.HBM)
    names = [jnp.asarray(t) for t in tables()]
    operands = [
        state, spec_weight1, spec_bias1, spec_weight2, spec_bias2, norm1_gain, norm1_bias, norm2_gain,
        norm2_bias, fc1_weight, fc1_bias, fc2_weight, fc2_bias, cotangent, *names,
    ]
    specs = [hbm] * len(operands)
    out = jax.ShapeDtypeStruct(state.shape, BF16)
    results = pl.pallas_call(
        kernel,
        out_shape=(out, out),
        in_specs=specs,
        out_specs=(vmem, vmem),
        scratch_shapes=[
            *[pltpu.VMEM(a.shape, a.dtype) for a in operands],
            pltpu.VMEM((8, NJ, 112, 128), BF16),
            pltpu.VMEM((8, NJ, 112, 128), BF16),
            pltpu.VMEM((8, NP, 56, 128), BF16),
            pltpu.VMEM((8, NP, 56, 128), BF16),
            pltpu.VMEM((2, TOK, D), F32),
            pltpu.VMEM((2, TOK, D), F32),
            pltpu.VMEM((2, TOK, D), F32),
            pltpu.VMEM((2 * TOK, FF), BF16),
            pltpu.VMEM((2 * TOK, FF), F32),
            pltpu.VMEM((TOK, D), F32),
            pltpu.VMEM((W, D), F32),
            pltpu.VMEM((16 * NP, D), F32),
            pltpu.VMEM((8 * H, 128), F32),
            pltpu.VMEM((4 * H, 128), F32),
            pltpu.VMEM((4 * H, 128), F32),
            pltpu.VMEM((ROWS, 256), F32),
            pltpu.VMEM((2, ROWS, 256), F32),
            pltpu.VMEM((2, ROWS, 256), F32),
            pltpu.VMEM((1, 256, 256), BF16),
            pltpu.VMEM((1, 256, 256), BF16),
            pltpu.VMEM((1, 256), F32),
            pltpu.VMEM((1, 256), F32),
            pltpu.VMEM((2, 4 * H, 2 * H), BF16),
            pltpu.VMEM((2 * H, 4 * H), BF16),
            pltpu.SemaphoreType.DMA((len(operands),)),
            pltpu.SemaphoreType.DMA((8,)),
            pltpu.SemaphoreType.DMA((8, NJ)),
            pltpu.SemaphoreType.DMA((8,)),
            pltpu.SemaphoreType.DMA((8, NP)),
        ],
        compiler_params=pltpu.CompilerParams(
            collective_id=0, has_side_effects=True, vmem_limit_bytes=67043328
        ),
        name="block",
    )(*operands)
    return pl.pallas_call(
        finish,
        out_shape=(out, out),
        in_specs=[vmem, vmem],
        out_specs=(vmem, vmem),
        compiler_params=pltpu.CompilerParams(vmem_limit_bytes=67043328),
        name="finish",
    )(*results)


def solution(mesh):
    in_specs = (
        P("ens", "lat", "lon", None),
        P(None, "lon", None, None),
        P(None, "lon", None),
        P(None, "lon", None, None),
        P(None, "lon", None),
        P(), P(), P(), P(), P(), P(), P(), P(),
        P("ens", "lat", "lon", None),
    )
    out_specs = (P("ens", "lat", "lon", None), P("ens", "lat", "lon", None))
    return jax.shard_map(shards, mesh=mesh, in_specs=in_specs, out_specs=out_specs, check_vma=False)
```

```python
import math

import jax
import jax.numpy as jnp
import numpy as np
from jax import lax
from jax.experimental import pallas as pl
from jax.experimental.pallas import tpu as pltpu
from jax.sharding import PartitionSpec as P

EPSILON = 1e-06
THRESHOLD = 0.01
F32 = jnp.float32
BF16 = jnp.bfloat16

NP = 16
NJ = 8
R = 6
C = 24
TOK = R * C
KS = 6
H = NP * R
W = NJ * C
BS = 96
D = 768
FF = 3072
HC = 512
ROWS = 2 * KS * H
FIRST, MIDDLE, LAST = [0, 5, 6], [1, 2, 3, 4, 7, 8, 10, 12, 13, 14, 15, 16, 17, 18], [11, 9]

roll = pltpu.roll


def tables():
    def cs(rows, cols, modulus):
        angle = 2.0 * np.pi * (np.outer(rows, cols) % modulus) / modulus
        return np.cos(angle) / math.sqrt(modulus), np.sin(angle) / math.sqrt(modulus)

    w = np.arange(W)
    cosine, sine = cs(w, np.arange(W // 2), W)
    parity = (1.0 - 2.0 * (w % 2)) / math.sqrt(W)
    ahead = np.zeros((NP, 16, W))
    even = np.zeros((W, NP, 16))
    odd = np.zeros((W, NP, 16))
    for p in range(NP):
        for kc in range(12):
            c, k = divmod(kc, KS)
            f = p * KS + k
            if c == 0:
                row, back = cosine[:, f], (2.0 if f else 1.0) * cosine[:, f]
            else:
                row, back = (-sine[:, f], -2.0 * sine[:, f]) if f else (parity, parity)
            ahead[p, kc] = row
            if kc < 8:
                even[:, p, kc] = back
                odd[:, p, kc] = back
            else:
                ahead[p, kc + 4] = row
                even[:, p, kc] = back
                odd[:, p, kc + 4] = back
    ahead = ahead.reshape(NP * 16, W)
    even = even.reshape(W, NP * 16)
    odd = odd.reshape(W, NP * 16)
    g = np.arange(H)
    co, si = cs(g, g, H)
    fwd = np.block([[co, si], [-si, co]])
    inv = 0.5 * np.block([[co, -si], [si, co]])
    return [split_table(ahead), split_table(fwd), rounded(even), rounded(odd), rounded(inv)]


def rounded(table):
    return np.asarray(table, np.float32).astype(jnp.bfloat16)


def split_table(table):
    high = np.asarray(table, np.float32).astype(jnp.bfloat16)
    low = (np.asarray(table, np.float64) - high.astype(np.float64)).astype(np.float32).astype(jnp.bfloat16)
    return np.stack([high, low])


def dot(a, b):
    return jnp.dot(a, b, preferred_element_type=F32)


def dot_nt(a, b):
    return lax.dot_general(a, b, (((1,), (1,)), ((), ())), preferred_element_type=F32)


def table_dot(table, x):
    x = x.astype(BF16)
    if len(table.shape) == 2:
        return dot(table[...], x)
    return dot(table[0], x) + dot(table[1], x)


def row(ref):
    return ref[...].reshape(1, -1)


def lanes():
    return lax.broadcasted_iota(jnp.int32, (1, 128), 1)


def layer_norm(values):
    average = jnp.mean(values, axis=-1, keepdims=True)
    centred = values - average
    inverse = lax.rsqrt(jnp.mean(centred * centred, axis=-1, keepdims=True) + EPSILON)
    return centred * inverse, inverse


def norm_backward(gradient, gain, normed, inverse):
    scaled = gradient * gain
    return inverse * (
        scaled
        - jnp.mean(scaled, axis=-1, keepdims=True)
        - normed * jnp.mean(scaled * normed, axis=-1, keepdims=True)
    )


def cumulative(values):
    return 0.5 * (1.0 + lax.erf(values * 0.7071067811865476))


def density(values):
    return jnp.exp(-0.5 * values * values) * 0.3989422804014327


def feature_block(tile, b):
    t, o = divmod(BS * b, 128)
    if o == 0:
        return tile(t)
    first = roll(tile(t), 128 - o, 1)
    if o == 32:
        return first
    return jnp.where(lanes() < 128 - o, first, roll(tile(t + 1), 128 - o, 1))


def joined_blocks(blocks):
    lane = lanes()
    tiles = []
    for q in (0, 4):
        one, two, three = roll(blocks[q + 1], 96, 1), roll(blocks[q + 2], 64, 1), roll(blocks[q + 3], 32, 1)
        tiles += [
            jnp.where(lane < 96, blocks[q], one),
            jnp.where(lane < 64, one, two),
            jnp.where(lane < 32, two, three),
        ]
    return jnp.concatenate(tiles, axis=1)


def pack_lon(m):
    lane = lanes()
    extra = m[112:144]
    parts = [jnp.where(lane < 96, m[32 * i : 32 * i + 32], roll(extra, 96 - 32 * i, 1) if i < 3 else extra) for i in range(3)]
    return jnp.concatenate(parts + [m[96:112]], axis=0)


def unpack_lon(m):
    lane = lanes()
    extra = jnp.where(
        lane < 32, roll(m[0:32], 32, 1), jnp.where(lane < 64, roll(m[32:64], 64, 1), roll(m[64:96], 96, 1))
    )
    return jnp.concatenate([m, extra], axis=0)


def pack_lat(t):
    lane = lanes()
    out = []
    for i in range(R):
        shift = 96 - 32 * (i % 3)
        out.append(jnp.where(lane < 96, t[i], roll(t[7 + i // 3], shift, 1)))
    return jnp.concatenate(out + [t[6]], axis=0)


def unpack_lat(m):
    lane = lanes()
    t = [m[8 * i : 8 * i + 8] for i in range(7)]
    for e in range(2):
        a, b, c = t[3 * e : 3 * e + 3]
        t.append(jnp.where(lane < 32, roll(a, 32, 1), jnp.where(lane < 64, roll(b, 64, 1), roll(c, 96, 1))))
    return t


def at(index, size, count=None, offset=0):
    return pl.ds(pl.multiple_of(index * size + offset, 8), count or size)


def width_ahead(froms, recv, wide, tall, ahead, tos, put):
    for group in froms:
        recv.wait(group)
        for j in group:
            m = unpack_lon(recv(j).astype(F32))
            for r in range(R):
                wide[at(j, C), 128 * r : 128 * r + 128] = m[C * r : C * r + C]
    tall[...] = table_dot(ahead, wide[...])
    upper = lax.broadcasted_iota(jnp.int32, (8, 1), 0) < 4
    for group in tos:
        for p in group:
            def rows(r, offset):
                return tall[at(p, 16, 8, offset), 128 * r : 128 * r + 128]
            t = [rows(r, 0) for r in range(R)]
            t += [jnp.where(upper, rows(2 * i, 8), rows(2 * i + 1, 8)) for i in range(3)]
            put(p, pack_lat(t))
        put.send(group)


def slot_rows(kc, eights, fours):
    if kc < 8:
        return eights, pl.ds(kc, H, stride=8)
    return fours, pl.ds(kc - 8, H, stride=4)


def height_ahead(froms, recv, eights, fours, wide, spec, fwd, fwd0):
    for group in froms:
        recv.wait(group)
        for p in group:
            t = unpack_lat(recv(p).astype(F32))
            eights[at(p, 48), :] = jnp.concatenate(t[:6], axis=0)
            fours[at(p, 24), :] = jnp.concatenate(t[6:], axis=0)
    for c in range(2):
        for k in range(KS):
            ref, rows = slot_rows(c * KS + k, eights, fours)
            wide[H * c : H * c + H, 128 * k : 128 * k + 128] = ref[rows, :]
    zero = table_dot(fwd0, wide[:, 0:128])
    rest = table_dot(fwd, wide[:, 128:])
    half = KS * H
    spec[0:H, 0:128] = zero[0:H]
    spec[0:H, 128:256] = zero[H : 2 * H]
    spec[half : half + H, 0:128] = zero[2 * H : 3 * H]
    spec[half : half + H, 128:256] = zero[3 * H :]
    for k in range(1, KS):
        real, imag = rest[0:H, 128 * (k - 1) : 128 * k], rest[H:, 128 * (k - 1) : 128 * k]
        spec[H * k : H * k + H, 0:128] = real
        spec[H * k : H * k + H, 128:256] = imag
        spec[half + H * k : half + H * k + H, 0:128] = real
        spec[half + H * k : half + H * k + H, 128:256] = -imag


def height_back(spec, eights, fours, wide, first, inv, inv0, tos, put):
    half = KS * H
    for i, (start, lane) in enumerate(((0, 0), (0, 128), (half, 0), (half, 128))):
        first[H * i : H * i + H, :] = spec[start : start + H, lane : lane + 128]
    for k in range(1, KS):
        low = spec[H * k : H * k + H, :]
        high = spec[half + H * k : half + H * k + H, :]
        wide[0:H, 128 * k : 128 * k + 128] = low[:, 0:128] + high[:, 0:128]
        wide[H : 2 * H, 128 * k : 128 * k + 128] = low[:, 128:] - high[:, 128:]
    zero = table_dot(inv0, first[...])
    rest = table_dot(inv, wide[:, 128:])
    for c in range(2):
        for k in range(KS):
            ref, rows = slot_rows(c * KS + k, eights, fours)
            values = zero[H * c : H * c + H] if k == 0 else rest[H * c : H * c + H, 128 * (k - 1) : 128 * k]
            ref[rows, :] = values
    for group in tos:
        for p in group:
            t = [eights[at(p, 48, 8, 8 * i), :] for i in range(6)]
            t += [fours[at(p, 24, 8, 8 * i), :] for i in range(3)]
            put(p, pack_lat(t))
        put.send(group)


def width_back(froms, recv, tall, wide, even, odd, tos, put):
    for group in froms:
        recv.wait(group)
        for p in group:
            t = unpack_lat(recv(p).astype(F32))
            for r in range(R):
                lane = 128 * (r // 2) + 384 * (r % 2)
                tall[at(p, 16, 8), lane : lane + 128] = t[r]
                tall[at(p, 16, 8, 8), lane : lane + 128] = t[6 + r // 2]
    wide[:, 0:384] = table_dot(even, tall[:, 0:384])
    wide[:, 384:768] = table_dot(odd, tall[:, 384:768])
    for group in tos:
        for j in group:
            m = [wide[at(j, C), 128 * (r // 2) + 384 * (r % 2) : 128 * (r // 2) + 384 * (r % 2) + 128] for r in range(R)]
            put(j, pack_lon(jnp.concatenate(m, axis=0)))
        put.send(group)


def gathered(recv):
    recv.wait(range(NJ // 2))
    recv.wait(range(NJ // 2))
    return joined_blocks([unpack_lon(recv(b).astype(F32))[:, 0:128] for b in range(NJ)])


def matrix_dot(values, matrix):
    return dot(values.astype(BF16), matrix[0])


CHUNK = 384


def spectral_ahead(spec, first_pre, squares, mat1, bias1, mat2, bias2):
    for i in range(ROWS // CHUNK):
        rows = slice(i * CHUNK, i * CHUNK + CHUNK)
        pre = matrix_dot(spec[rows, :], mat1) + bias1[...]
        first_pre[rows, :] = pre
        second = matrix_dot(pre * cumulative(pre), mat2) + bias2[...]
        slope = jnp.tanh(second * (1.0 / THRESHOLD))
        squares[rows, :] = slope * slope
        spec[rows, :] = second - THRESHOLD * slope


def spectral_slopes(first_pre):
    for i in range(ROWS // CHUNK):
        rows = slice(i * CHUNK, i * CHUNK + CHUNK)
        pre = first_pre[rows, :]
        first_pre[rows, :] = cumulative(pre) + pre * density(pre)


def spectral_adjoint(spec, slopes, squares, mat1, mat2):
    for i in range(ROWS // CHUNK):
        rows = slice(i * CHUNK, i * CHUNK + CHUNK)
        grad = matrix_dot(spec[rows, :] * squares[rows, :], mat2)
        spec[rows, :] = matrix_dot(grad * slopes[rows, :], mat1)


def fill_matrix(out, weight):
    out[...] = jnp.zeros_like(out)
    real, imag = weight[0, 0], weight[1, 0]
    out[0, 0:BS, 0:BS] = real.astype(BF16)
    out[0, 0:BS, 128 : 128 + BS] = imag.astype(BF16)
    out[0, 128 : 128 + BS, 0:BS] = (-imag).astype(BF16)
    out[0, 128 : 128 + BS, 128 : 128 + BS] = real.astype(BF16)


def fill_first(fwd0, inv0, fwd, inv, packed):
    left = lax.broadcasted_iota(jnp.int32, (1, 2 * H), 1) < H
    one = jnp.where(packed, 0.0, 1.0)
    first = jnp.where(left, 1.0, one)
    second = jnp.where(left, one, 1.0)
    for i in range(2):
        real, imag = fwd[i, 0:H].astype(F32), fwd[i, H : 2 * H].astype(F32)
        fwd0[i, 0:H] = (real * first).astype(BF16)
        fwd0[i, H : 2 * H] = (imag * first).astype(BF16)
        fwd0[i, 2 * H : 3 * H] = (jnp.where(packed, imag, real) * second).astype(BF16)
        fwd0[i, 3 * H : 4 * H] = (-jnp.where(packed, real, imag) * second).astype(BF16)
    real, imag = inv[0:H].astype(F32), inv[H : 2 * H].astype(F32)
    sign = jnp.where(left, 1.0, -1.0)
    inv0[0:H, 0 : 2 * H] = jnp.where(packed, 2.0 * real, real).astype(BF16)
    inv0[H : 2 * H, 0 : 2 * H] = (imag * one).astype(BF16)
    inv0[0:H, 2 * H : 4 * H] = (real * sign * one).astype(BF16)
    inv0[H : 2 * H, 2 * H : 4 * H] = jnp.where(packed, 2.0 * real, imag * sign).astype(BF16)


def fill_transposed(out, matrix):
    n = out.shape[-1]
    one = lax.broadcasted_iota(jnp.int32, (n, n), 0) == lax.broadcasted_iota(jnp.int32, (n, n), 1)
    out[0] = dot_nt(jnp.where(one, 1.0, 0.0).astype(BF16), matrix[0]).astype(BF16)


def fill_bias(out, bias):
    out[...] = jnp.zeros_like(out)
    out[0:1, 0:BS] = bias[0]
    out[0:1, 128 : 128 + BS] = bias[1]


def token_ahead(loop, mixed, cot, held, fc1, bias1, gain2, shift2, hidden, gh, acc):
    normed, inverse = layer_norm(mixed)
    v = (normed * gain2 + shift2).astype(BF16)
    for n in range(FF // HC):
        cols = slice(n * HC, n * HC + HC)
        pre = dot(v, fc1[:, cols]) + bias1[cols].reshape(1, -1)
        phi = cumulative(pre)
        hidden[held, cols] = (pre * phi).astype(BF16)
        grad = (gh[held, cols] * (phi + pre * density(pre))).astype(BF16)
        if n:
            acc[...] += dot_nt(grad, fc1[:, cols])
        else:
            acc[...] = dot_nt(grad, fc1[:, cols])
    return (cot + norm_backward(acc[...], gain2, normed, inverse)).astype(BF16).astype(F32)


def kernel(
    *refs,
):
    sources, rest = refs[:19], refs[19:]
    (
        advanced_hbm, sensitivity_hbm,
        advanced, sensitivity, state, weight1, bias_1, weight2, bias_2, gain1, shift1, gain2, shift2, fc1, fc1_bias, fc2, fc2_bias, cotangent,
        ahead, fwd, even, odd, inv,
        lon_send, lon_recv, lat_send, lat_recv, lowered, mixed, grads, hidden, gh, acc,
        wide, tall, eights, fours, first, spec, first_pre, squares, mat1, mat2, turned1, turned2, bias1, bias2, fwd0, inv0,
        load_sem, store_sem, lon_send_sem, lon_recv_sem, lat_send_sem, lat_recv_sem,
    ) = rest
    p = lax.axis_index("lat")
    j = lax.axis_index("lon")

    def loop(count, body):
        lax.fori_loop(0, count, lambda i, _: (body(i), 0)[1], 0)

    ens = lax.axis_index("ens")
    lon_ring = [(dx, dy) for dx in (2, 1, 3, 0) for dy in (0, 1)]
    lat_ring = [(dz, dc) for dz in (4, 3, 5, 2, 6, 1, 7, 0) for dc in (0, 1)]

    def lon_peers(sign):
        return [lax.rem(j // 2 + 4 + sign * dx, 4) * 2 + lax.rem(j + dy, 2) for dx, dy in lon_ring]

    def lat_peers(sign):
        return [lax.rem(p // 2 + 8 + sign * dz, 8) * 2 + lax.rem(p + dc, 2) for dz, dc in lat_ring if dz + dc]

    lon_to, lon_from, lat_to, lat_from = lon_peers(1), lon_peers(-1), lat_peers(1), lat_peers(-1)

    def device(axis, to):
        return {"lon": to, "ens": 1 - ens} if axis == "lon" else {"lat": to}

    barrier = pltpu.get_barrier_semaphore()
    for axis, peers in (("lat", lat_to), ("lon", lon_to)):
        for to in peers:
            pl.semaphore_signal(barrier, inc=1, device_id=device(axis, to), device_id_type=pl.DeviceIdType.MESH)
    held_here = (
        state, weight1, bias_1, weight2, bias_2, gain1, shift1, gain2, shift2, fc1, fc1_bias, fc2, fc2_bias, cotangent,
        ahead, fwd, even, odd, inv,
    )
    loads = [pltpu.make_async_copy(a, b, load_sem.at[i]) for i, (a, b) in enumerate(zip(sources, held_here))]
    for i in FIRST + MIDDLE + LAST:
        loads[i].start()
    for i in FIRST:
        loads[i].wait()

    def buffers(x, s, axis):
        e = 2 * x + s
        if axis == "lon":
            return lon_send, lon_recv, lon_send_sem, lon_recv_sem, e, j
        return lat_send, lat_recv, lat_send_sem, lat_recv_sem, e, p

    def copy(x, s, axis, to, half):
        send, recv, send_sem, recv_sem, e, me = buffers(x, s, axis)
        return pltpu.make_async_remote_copy(
            src_ref=send.at[e, to],
            dst_ref=recv.at[e, me],
            send_sem=send_sem.at[e],
            recv_sem=recv_sem.at[e, half],
            device_id=device(axis, to),
            device_id_type=pl.DeviceIdType.MESH,
        )

    def several(x, s, axis, count, half):
        send, recv, send_sem, recv_sem, e, me = buffers(x, s, axis)
        return pltpu.make_async_remote_copy(
            src_ref=send.at[e, pl.ds(0, count)],
            dst_ref=recv.at[e, pl.ds(0, count)],
            send_sem=send_sem.at[e],
            recv_sem=recv_sem.at[e, half],
            device_id=device(axis, lon_to[0] if axis == "lon" else lat_to[0]),
            device_id_type=pl.DeviceIdType.MESH,
        )

    class Sender:
        def __init__(self, x, s, axis):
            self.where, self.half = (x, s, axis), 0

        def __call__(self, to, values):
            send, recv, _, _, e, _ = buffers(*self.where)
            (recv if to is p else send)[e, to] = values.astype(BF16)

        def send(self, group):
            for to in group:
                if to is not p:
                    copy(*self.where, to, self.half).start()
            self.half += 1

    class Receiver:
        def __init__(self, x, s, axis):
            self.where, self.half = (x, s, axis), 0

        def wait(self, group):
            several(*self.where, len([0 for source in group if source is not p]), self.half).wait_recv()
            self.half += 1

        def __call__(self, source):
            _, recv, _, _, e, _ = buffers(*self.where)
            return recv[e, source]

    sender, receiver = Sender, Receiver
    lon_tos, lon_froms = [lon_to[:4], lon_to[4:]], [lon_from[:4], lon_from[4:]]
    lat_tos, lat_froms = [lat_to[:8], lat_to[8:] + [p]], [[p] + lat_from[:8], lat_from[8:]]

    def tokens(ref, s):
        return jnp.concatenate([ref[s, r].astype(F32) for r in range(R)], axis=0)

    def out_tokens(ref, s, values):
        for r in range(R):
            ref[s, r] = values[C * r : C * r + C].astype(BF16)

    def held(s):
        return slice(TOK * s, TOK * s + TOK)

    def send_tokens(x, s, ref):
        e = 2 * x + s
        for b in range(NJ):
            lon_send[e, b] = pack_lon(feature_block(lambda t: ref[s, :, 128 * t : 128 * t + 128], b)).astype(BF16)
        if e == 0:
            pl.semaphore_wait(barrier, NP - 1 + NJ)
        for half in range(2):
            for to in lon_tos[half]:
                copy(x, s, "lon", to, half).start()

    for s in range(2):
        with jax.named_scope("ln"):
            normed, _ = layer_norm(tokens(state, s))
            lowered[s] = (normed * row(gain1) + row(shift1)).astype(BF16).astype(F32)
            send_tokens(0, s, lowered)
    for i in MIDDLE:
        loads[i].wait()
    fill_matrix(mat1, weight1)
    fill_matrix(mat2, weight2)
    fill_transposed(turned1, mat1)
    fill_transposed(turned2, mat2)
    fill_bias(bias1, bias_1)
    fill_bias(bias2, bias_2)
    fill_first(fwd0, inv0, fwd, inv, p == 0)

    for s in range(2):
        with jax.named_scope("w0"):
            width_ahead(lon_froms, receiver(0, s, "lon"), wide, tall, ahead, lat_tos, sender(0, s, "lat"))

    with jax.named_scope("gh"):
        loads[11].wait()
        cots = jnp.concatenate([tokens(cotangent, s) for s in range(2)], axis=0).astype(BF16)

        def cot_step(n):
            cols = pl.ds(pl.multiple_of(n * HC, HC), HC)
            gh[:, cols] = dot_nt(cots, fc2[cols, :])
        loop(FF // HC, cot_step)

    for s in range(2):
        with jax.named_scope("h0"):
            height_ahead(lat_froms, receiver(0, s, "lat"), eights, fours, wide, spec, fwd, fwd0)
        with jax.named_scope("sp0"):
            spectral_ahead(spec, first_pre.at[s], squares.at[s], mat1, bias1, mat2, bias2)
        with jax.named_scope("hb1"):
            height_back(spec, eights, fours, wide, first, inv, inv0, lat_tos, sender(1, s, "lat"))
    for s in range(2):
        with jax.named_scope("slopes"):
            spectral_slopes(first_pre.at[s])
    loads[9].wait()
    for s in range(2):
        with jax.named_scope("wb1"):
            width_back(lat_froms, receiver(1, s, "lat"), tall, wide, even, odd, lon_tos, sender(1, s, "lon"))
    for s in range(2):
        with jax.named_scope("gath1"):
            filtered = gathered(receiver(1, s, "lon"))
            mixed[s] = (filtered + lowered[s] + tokens(state, s)).astype(BF16).astype(F32)
        with jax.named_scope("token"):
            grads[s] = token_ahead(
                loop, mixed[s], tokens(cotangent, s), held(s), fc1, fc1_bias, row(gain2), row(shift2), hidden, gh, acc
            )
        with jax.named_scope("sendt"):
            send_tokens(2, s, grads)

    def store(i, s):
        source, target = ((advanced, advanced_hbm), (sensitivity, sensitivity_hbm))[i]
        return pltpu.make_async_copy(source.at[s], target.at[s], store_sem.at[2 * i + s])

    def advance(s):
        for n in range(D // 256):
            cols = slice(256 * n, 256 * n + 256)
            values = dot(hidden[TOK * s : TOK * s + TOK, :], fc2[:, cols]) + fc2_bias[cols].reshape(1, -1) + mixed[s, :, cols]
            for r in range(R):
                advanced[s, r, :, cols] = values[C * r : C * r + C].astype(BF16)

    for s in range(2):
        with jax.named_scope("w2"):
            width_ahead(lon_froms, receiver(2, s, "lon"), wide, tall, ahead, lat_tos, sender(2, s, "lat"))
    for s in range(2):
        with jax.named_scope("adv"):
            advance(s)
        store(0, s).start()
    for s in range(2):
        with jax.named_scope("h2"):
            height_ahead(lat_froms, receiver(2, s, "lat"), eights, fours, wide, spec, fwd, fwd0)
        with jax.named_scope("sp2"):
            spectral_adjoint(spec, first_pre.at[s], squares.at[s], turned1, turned2)
        with jax.named_scope("hb3"):
            height_back(spec, eights, fours, wide, first, inv, inv0, lat_tos, sender(3, s, "lat"))
    for s in range(2):
        with jax.named_scope("wb3"):
            width_back(lat_froms, receiver(3, s, "lat"), tall, wide, even, odd, lon_tos, sender(3, s, "lon"))
    for s in range(2):
        with jax.named_scope("final"):
            grad = grads[s]
            grad_lowered = gathered(receiver(3, s, "lon")) + grad
            normed, inverse = layer_norm(tokens(state, s))
            out_tokens(sensitivity, s, grad + norm_backward(grad_lowered, row(gain1), normed, inverse))
        store(1, s).start()
    with jax.named_scope("tail_sent"):
        for x in range(4):
            for s in range(2):
                several(x, s, "lon", NJ, 0).wait_send()
                several(x, s, "lat", NP - 1, 0).wait_send()
    with jax.named_scope("tail_store"):
        for i in range(2):
            for s in range(2):
                store(i, s).wait()


def finish(advanced, sensitivity, advanced_out, sensitivity_out):
    advanced_out[...] = advanced[...]
    sensitivity_out[...] = sensitivity[...]


def shards(
    state, spec_weight1, spec_bias1, spec_weight2, spec_bias2, norm1_gain, norm1_bias, norm2_gain, norm2_bias,
    fc1_weight, fc1_bias, fc2_weight, fc2_bias, cotangent,
):
    vmem = pl.BlockSpec(memory_space=pltpu.VMEM)
    hbm = pl.BlockSpec(memory_space=pltpu.HBM)
    names = [jnp.asarray(t) for t in tables()]
    operands = [
        state, spec_weight1, spec_bias1, spec_weight2, spec_bias2, norm1_gain, norm1_bias, norm2_gain,
        norm2_bias, fc1_weight, fc1_bias, fc2_weight, fc2_bias, cotangent, *names,
    ]
    specs = [hbm] * len(operands)
    out = jax.ShapeDtypeStruct(state.shape, BF16)
    results = pl.pallas_call(
        kernel,
        out_shape=(out, out),
        in_specs=specs,
        out_specs=(hbm, hbm),
        scratch_shapes=[
            pltpu.VMEM(state.shape, BF16),
            pltpu.VMEM(state.shape, BF16),
            *[pltpu.VMEM(a.shape, a.dtype) for a in operands],
            pltpu.VMEM((8, NJ, 112, 128), BF16),
            pltpu.VMEM((8, NJ, 112, 128), BF16),
            pltpu.VMEM((8, NP, 56, 128), BF16),
            pltpu.VMEM((8, NP, 56, 128), BF16),
            pltpu.VMEM((2, TOK, D), F32),
            pltpu.VMEM((2, TOK, D), F32),
            pltpu.VMEM((2, TOK, D), F32),
            pltpu.VMEM((2 * TOK, FF), BF16),
            pltpu.VMEM((2 * TOK, FF), F32),
            pltpu.VMEM((TOK, D), F32),
            pltpu.VMEM((W, D), F32),
            pltpu.VMEM((16 * NP, D), F32),
            pltpu.VMEM((8 * H, 128), F32),
            pltpu.VMEM((4 * H, 128), F32),
            pltpu.VMEM((4 * H, 128), F32),
            pltpu.VMEM((ROWS, 256), F32),
            pltpu.VMEM((2, ROWS, 256), F32),
            pltpu.VMEM((2, ROWS, 256), F32),
            pltpu.VMEM((1, 256, 256), BF16),
            pltpu.VMEM((1, 256, 256), BF16),
            pltpu.VMEM((1, 256, 256), BF16),
            pltpu.VMEM((1, 256, 256), BF16),
            pltpu.VMEM((1, 256), F32),
            pltpu.VMEM((1, 256), F32),
            pltpu.VMEM((2, 4 * H, 2 * H), BF16),
            pltpu.VMEM((2 * H, 4 * H), BF16),
            pltpu.SemaphoreType.DMA((len(operands),)),
            pltpu.SemaphoreType.DMA((4,)),
            pltpu.SemaphoreType.DMA((8,)),
            pltpu.SemaphoreType.DMA((8, 2)),
            pltpu.SemaphoreType.DMA((8,)),
            pltpu.SemaphoreType.DMA((8, 2)),
        ],
        compiler_params=pltpu.CompilerParams(
            collective_id=0, has_side_effects=True, vmem_limit_bytes=67043328
        ),
        name="block",
    )(*operands)
    return pl.pallas_call(
        finish,
        out_shape=(out, out),
        in_specs=[vmem, vmem],
        out_specs=(vmem, vmem),
        compiler_params=pltpu.CompilerParams(vmem_limit_bytes=67043328),
        name="finish",
    )(*results)


def solution(mesh):
    in_specs = (
        P("ens", "lat", "lon", None),
        P(None, "lon", None, None),
        P(None, "lon", None),
        P(None, "lon", None, None),
        P(None, "lon", None),
        P(), P(), P(), P(), P(), P(), P(), P(),
        P("ens", "lat", "lon", None),
    )
    out_specs = (P("ens", "lat", "lon", None), P("ens", "lat", "lon", None))
    return jax.shard_map(shards, mesh=mesh, in_specs=in_specs, out_specs=out_specs, check_vma=False)
```

```python
import math

import jax
import jax.numpy as jnp
import numpy as np
from jax import lax
from jax.experimental import pallas as pl
from jax.experimental.pallas import tpu as pltpu
from jax.sharding import PartitionSpec as P

EPSILON = 1e-06
THRESHOLD = 0.01
F32 = jnp.float32
BF16 = jnp.bfloat16

NP = 16
NJ = 8
R = 6
C = 24
TOK = R * C
KS = 6
H = NP * R
W = NJ * C
BS = 96
D = 768
FF = 3072
HC = 512
ROWS = 2 * KS * H
FIRST, MIDDLE, LAST = [5, 6], [1, 2, 3, 4, 7, 8, 10, 12, 13, 14, 15, 16, 17, 18], [11, 9]

roll = pltpu.roll


def tables():
    def cs(rows, cols, modulus):
        angle = 2.0 * np.pi * (np.outer(rows, cols) % modulus) / modulus
        return np.cos(angle) / math.sqrt(modulus), np.sin(angle) / math.sqrt(modulus)

    w = np.arange(W)
    cosine, sine = cs(w, np.arange(W // 2), W)
    parity = (1.0 - 2.0 * (w % 2)) / math.sqrt(W)
    ahead = np.zeros((NP, 16, W))
    even = np.zeros((W, NP, 16))
    odd = np.zeros((W, NP, 16))
    for p in range(NP):
        for kc in range(12):
            c, k = divmod(kc, 4) if kc < 8 else ((kc - 8) // 2, 4 + kc % 2)
            f = p * KS + k
            if c == 0:
                row, back = cosine[:, f], (2.0 if f else 1.0) * cosine[:, f]
            else:
                row, back = (-sine[:, f], -2.0 * sine[:, f]) if f else (parity, parity)
            ahead[p, kc] = row
            if kc < 8:
                even[:, p, kc] = back
                odd[:, p, kc] = back
            else:
                ahead[p, kc + 4] = row
                even[:, p, kc] = back
                odd[:, p, kc + 4] = back
    ahead = ahead.reshape(NP * 16, W)
    even = even.reshape(W, NP * 16)
    odd = odd.reshape(W, NP * 16)
    g = np.arange(H)
    co, si = cs(g, g, H)
    fwd = np.block([[co, si], [-si, co]])
    inv = 0.5 * np.block([[co, -si], [si, co]])
    return [split_table(ahead), split_table(fwd), rounded(even), rounded(odd), rounded(inv)]


def rounded(table):
    return np.asarray(table, np.float32).astype(jnp.bfloat16)


def split_table(table):
    high = np.asarray(table, np.float32).astype(jnp.bfloat16)
    low = (np.asarray(table, np.float64) - high.astype(np.float64)).astype(np.float32).astype(jnp.bfloat16)
    return np.stack([high, low])


def dot(a, b):
    return jnp.dot(a, b, preferred_element_type=F32)


def dot_nt(a, b):
    return lax.dot_general(a, b, (((1,), (1,)), ((), ())), preferred_element_type=F32)


def table_dot(table, x):
    x = x.astype(BF16)
    if len(table.shape) == 2:
        return dot(table[...], x)
    return dot(table[0], x) + dot(table[1], x)


def row(ref):
    return ref[...].reshape(1, -1)


def lanes():
    return lax.broadcasted_iota(jnp.int32, (1, 128), 1)


def layer_norm(values):
    average = jnp.mean(values, axis=-1, keepdims=True)
    centred = values - average
    inverse = lax.rsqrt(jnp.mean(centred * centred, axis=-1, keepdims=True) + EPSILON)
    return centred * inverse, inverse


def norm_backward(gradient, gain, normed, inverse):
    scaled = gradient * gain
    return inverse * (
        scaled
        - jnp.mean(scaled, axis=-1, keepdims=True)
        - normed * jnp.mean(scaled * normed, axis=-1, keepdims=True)
    )


def cumulative(values):
    return 0.5 * (1.0 + lax.erf(values * 0.7071067811865476))


def density(values):
    return jnp.exp(-0.5 * values * values) * 0.3989422804014327


def feature_block(tile, b):
    t, o = divmod(BS * b, 128)
    if o == 0:
        return tile(t)
    first = roll(tile(t), 128 - o, 1)
    if o == 32:
        return first
    return jnp.where(lanes() < 128 - o, first, roll(tile(t + 1), 128 - o, 1))


def joined_blocks(blocks):
    lane = lanes()
    tiles = []
    for q in (0, 4):
        one, two, three = roll(blocks[q + 1], 96, 1), roll(blocks[q + 2], 64, 1), roll(blocks[q + 3], 32, 1)
        tiles += [
            jnp.where(lane < 96, blocks[q], one),
            jnp.where(lane < 64, one, two),
            jnp.where(lane < 32, two, three),
        ]
    return jnp.concatenate(tiles, axis=1)


def pack_lon(m):
    lane = lanes()
    extra = m[112:144]
    parts = [jnp.where(lane < 96, m[32 * i : 32 * i + 32], roll(extra, 96 - 32 * i, 1) if i < 3 else extra) for i in range(3)]
    return jnp.concatenate(parts + [m[96:112]], axis=0)


def unpack_lon(m):
    lane = lanes()
    extra = jnp.where(
        lane < 32, roll(m[0:32], 32, 1), jnp.where(lane < 64, roll(m[32:64], 64, 1), roll(m[64:96], 96, 1))
    )
    return jnp.concatenate([m, extra], axis=0)


def beside(tile, extra, i):
    return jnp.where(lanes() < 96, tile, roll(extra, 96 - 32 * i, 1))


def from_beside(a, b, c):
    lane = lanes()
    return jnp.where(lane < 32, roll(a, 32, 1), jnp.where(lane < 64, roll(b, 64, 1), roll(c, 96, 1)))


OUT, BACK = 40, 32


def pack_out(part, a, c):
    if part == 0:
        tiles = [beside(a[i], a[5], i) for i in range(3)] + [beside(a[3], c[2], 0), beside(a[4], c[2], 1)]
    else:
        tiles = [beside(c[0], c[2], 2), c[1]]
    return jnp.concatenate(tiles, axis=0)


def unpack_out(part, t):
    if part == 0:
        return t[:5] + [from_beside(*t[:3])]
    return [t[5], t[6], from_beside(t[3], t[4], t[5])]


def pack_back(part, a, c):
    if part == 0:
        tiles = [beside(a[i], a[4], i) for i in range(3)] + [beside(a[3], a[5], 0)]
    else:
        tiles = [beside(c[0], a[5], 1), beside(c[1], a[5], 2), c[2]]
    return jnp.concatenate(tiles, axis=0)


def eight_rows(m):
    return [m[8 * i : 8 * i + 8] for i in range(m.shape[0] // 8)]


def at(index, size, count=None, offset=0):
    return pl.ds(pl.multiple_of(index * size + offset, 8), count or size)


def width_ahead(froms, recv, wide, tall, ahead, tos, put):
    for half, group in enumerate(froms):
        recv.wait(len(group), 0, 112, half)
        for j in group:
            m = unpack_lon(recv(j).astype(F32))
            for r in range(R):
                wide[at(j, C), 128 * r : 128 * r + 128] = m[C * r : C * r + C]
    tall[...] = table_dot(ahead, wide[...])
    upper = lax.broadcasted_iota(jnp.int32, (8, 1), 0) < 4

    def tile(p, r, offset):
        return tall[at(p, 16, 8, offset), 128 * r : 128 * r + 128]

    def fours(p, i):
        return jnp.where(upper, tile(p, 2 * i, 8), tile(p, 2 * i + 1, 8))

    for group in tos:
        for p in group:
            put(p, pack_out(0, [tile(p, r, 0) for r in range(R)], [None, None, fours(p, 2)]))
        put.send(group, 0, OUT, 0)
    for group in tos:
        for p in group:
            put(p, pack_out(1, None, [fours(p, i) for i in range(3)]), OUT)
        put.send(group, OUT, 56 - OUT, 1)


def slot_rows(c, k, eights, fours):
    if k < 4:
        return eights, pl.ds(4 * c + k, H, stride=8)
    return fours, pl.ds(2 * c + k - 4, H, stride=4)


def spec_rows(k, high):
    start = H * (k + 4 * high) if k < 4 else H * (8 + (k - 4) + 2 * high)
    return slice(start, start + H)


PARTS = ((0, 8 * H), (8 * H, 12 * H))
SLOTS = ((0, 1, 2, 3), (4, 5))


def height_ahead(part, froms, recv, eights, fours, spec, fwd, fwd0):
    recv.wait(NP - 1, *((0, OUT), (OUT, 56 - OUT))[part], part)
    for p in froms:
        t = unpack_out(part, eight_rows(recv(p, 0, 56 if part else OUT).astype(F32)))
        if part == 0:
            eights[at(p, 48), :] = jnp.concatenate(t, axis=0)
        else:
            fours[at(p, 24), :] = jnp.concatenate(t, axis=0)

    def column(k):
        pair = [slot_rows(c, k, eights, fours) for c in range(2)]
        return jnp.concatenate([ref[rows, :] for ref, rows in pair], axis=0).astype(BF16)

    slots = SLOTS[part]
    if part == 0:
        zero = table_dot(fwd0, column(0))
        for i in range(4):
            spec[spec_rows(0, i // 2), 128 * (i % 2) : 128 * (i % 2) + 128] = zero[H * i : H * i + H]
        slots = slots[1:]
    rest = table_dot(fwd, jnp.concatenate([column(k) for k in slots], axis=1))
    for i, k in enumerate(slots):
        real, imag = rest[0:H, 128 * i : 128 * i + 128], rest[H:, 128 * i : 128 * i + 128]
        for high in range(2):
            spec[spec_rows(k, high), 0:128] = real
            spec[spec_rows(k, high), 128:256] = -imag if high else imag


def height_back(part, spec, eights, fours, inv, inv0, tos, put):
    def column(k):
        low, high = spec[spec_rows(k, 0), :], spec[spec_rows(k, 1), :]
        real, imag = low[:, 0:128] + high[:, 0:128], low[:, 128:] - high[:, 128:]
        return jnp.concatenate([real, imag], axis=0).astype(BF16)

    def keep(k, values):
        for c in range(2):
            ref, rows = slot_rows(c, k, eights, fours)
            ref[rows, :] = values[H * c : H * c + H]

    slots = SLOTS[part]
    if part == 0:
        places = [spec[spec_rows(0, i // 2), 128 * (i % 2) : 128 * (i % 2) + 128] for i in range(4)]
        keep(0, table_dot(inv0, jnp.concatenate(places, axis=0)))
        slots = slots[1:]
    rest = table_dot(inv, jnp.concatenate([column(k) for k in slots], axis=1))
    for i, k in enumerate(slots):
        keep(k, rest[:, 128 * i : 128 * i + 128])
    for group in tos:
        for p in group:
            a = [eights[at(p, 48, 8, 8 * i), :] for i in range(6)]
            c = [fours[at(p, 24, 8, 8 * i), :] for i in range(3)] if part else None
            put(p, pack_back(part, a, c), BACK * part)
        put.send(group, *((0, BACK), (BACK, 56 - BACK))[part], part)


def width_back(froms, recv, tall, wide, even, odd, tos, put):
    def keep(p, r, offset, tile):
        lane = 128 * (r // 2) + 384 * (r % 2)
        tall[at(p, 16, 8, offset), lane : lane + 128] = tile

    recv.wait(NP - 1, 0, BACK, 0)
    for p in froms:
        t = eight_rows(recv(p, 0, BACK).astype(F32))
        for r, tile in enumerate(t + [from_beside(*t[:3])]):
            keep(p, r, 0, tile)
    recv.wait(NP - 1, BACK, 56 - BACK, 1)
    for p in froms:
        t = eight_rows(recv(p, BACK - 8, 64 - BACK).astype(F32))
        keep(p, 5, 0, from_beside(*t[:3]))
        for r in range(R):
            keep(p, r, 8, t[1 + r // 2])
    wide[:, 0:384] = table_dot(even, tall[:, 0:384])
    wide[:, 384:768] = table_dot(odd, tall[:, 384:768])
    for half, group in enumerate(tos):
        for j in group:
            m = [wide[at(j, C), 128 * (r // 2) + 384 * (r % 2) : 128 * (r // 2) + 384 * (r % 2) + 128] for r in range(R)]
            put(j, pack_lon(jnp.concatenate(m, axis=0)))
        put.send(group, 0, 112, half)


def gathered(recv):
    for half in range(2):
        recv.wait(NJ // 2, 0, 112, half)
    return joined_blocks([unpack_lon(recv(b).astype(F32))[:, 0:128] for b in range(NJ)])


def matrix_dot(values, matrix):
    return dot(values.astype(BF16), matrix[0])


CHUNK = 384


def spectral_ahead(part, spec, first_pre, squares, mat1, bias1, mat2, bias2):
    for start in range(*PARTS[part], CHUNK):
        rows = slice(start, start + CHUNK)
        pre = matrix_dot(spec[rows, :], mat1) + bias1[...]
        first_pre[rows, :] = pre
        second = matrix_dot(pre * cumulative(pre), mat2) + bias2[...]
        slope = jnp.tanh(second * (1.0 / THRESHOLD))
        squares[rows, :] = slope * slope
        spec[rows, :] = second - THRESHOLD * slope


def spectral_slopes(first_pre):
    for i in range(ROWS // CHUNK):
        rows = slice(i * CHUNK, i * CHUNK + CHUNK)
        pre = first_pre[rows, :]
        first_pre[rows, :] = cumulative(pre) + pre * density(pre)


def spectral_adjoint(part, spec, slopes, squares, mat1, mat2):
    for start in range(*PARTS[part], CHUNK):
        rows = slice(start, start + CHUNK)
        grad = matrix_dot(spec[rows, :] * squares[rows, :], mat2)
        spec[rows, :] = matrix_dot(grad * slopes[rows, :], mat1)


def fill_matrix(out, weight):
    out[...] = jnp.zeros_like(out)
    real, imag = weight[0, 0], weight[1, 0]
    out[0, 0:BS, 0:BS] = real.astype(BF16)
    out[0, 0:BS, 128 : 128 + BS] = imag.astype(BF16)
    out[0, 128 : 128 + BS, 0:BS] = (-imag).astype(BF16)
    out[0, 128 : 128 + BS, 128 : 128 + BS] = real.astype(BF16)


def fill_first(fwd0, inv0, fwd, inv, packed):
    left = lax.broadcasted_iota(jnp.int32, (1, 2 * H), 1) < H
    one = jnp.where(packed, 0.0, 1.0)
    first = jnp.where(left, 1.0, one)
    second = jnp.where(left, one, 1.0)
    for i in range(2):
        real, imag = fwd[i, 0:H].astype(F32), fwd[i, H : 2 * H].astype(F32)
        fwd0[i, 0:H] = (real * first).astype(BF16)
        fwd0[i, H : 2 * H] = (imag * first).astype(BF16)
        fwd0[i, 2 * H : 3 * H] = (jnp.where(packed, imag, real) * second).astype(BF16)
        fwd0[i, 3 * H : 4 * H] = (-jnp.where(packed, real, imag) * second).astype(BF16)
    real, imag = inv[0:H].astype(F32), inv[H : 2 * H].astype(F32)
    sign = jnp.where(left, 1.0, -1.0)
    inv0[0:H, 0 : 2 * H] = jnp.where(packed, 2.0 * real, real).astype(BF16)
    inv0[H : 2 * H, 0 : 2 * H] = (imag * one).astype(BF16)
    inv0[0:H, 2 * H : 4 * H] = (real * sign * one).astype(BF16)
    inv0[H : 2 * H, 2 * H : 4 * H] = jnp.where(packed, 2.0 * real, imag * sign).astype(BF16)


def fill_transposed(out, matrix):
    n = out.shape[-1]
    one = lax.broadcasted_iota(jnp.int32, (n, n), 0) == lax.broadcasted_iota(jnp.int32, (n, n), 1)
    out[0] = dot_nt(jnp.where(one, 1.0, 0.0).astype(BF16), matrix[0]).astype(BF16)


def fill_bias(out, bias):
    out[...] = jnp.zeros_like(out)
    out[0:1, 0:BS] = bias[0]
    out[0:1, 128 : 128 + BS] = bias[1]


def token_ahead(loop, mixed, cot, held, fc1, bias1, gain2, shift2, hidden, gh, acc):
    normed, inverse = layer_norm(mixed)
    v = (normed * gain2 + shift2).astype(BF16)
    for n in range(FF // HC):
        cols = slice(n * HC, n * HC + HC)
        pre = dot(v, fc1[:, cols]) + bias1[cols].reshape(1, -1)
        phi = cumulative(pre)
        hidden[held, cols] = (pre * phi).astype(BF16)
        grad = (gh[held, cols] * (phi + pre * density(pre))).astype(BF16)
        if n:
            acc[...] += dot_nt(grad, fc1[:, cols])
        else:
            acc[...] = dot_nt(grad, fc1[:, cols])
    return (cot + norm_backward(acc[...], gain2, normed, inverse)).astype(BF16).astype(F32)


def kernel(
    *refs,
):
    sources, rest = refs[:19], refs[19:]
    (
        advanced_hbm, sensitivity_hbm,
        advanced, sensitivity, state, weight1, bias_1, weight2, bias_2, gain1, shift1, gain2, shift2, fc1, fc1_bias, fc2, fc2_bias, cotangent,
        ahead, fwd, even, odd, inv,
        lon_send, lon_recv, lat_send, lat_recv, lowered, mixed, grads, hidden, gh, acc,
        wide, tall, eights, fours, spec, first_pre, squares, mat1, mat2, turned1, turned2, bias1, bias2, fwd0, inv0,
        load_sem, store_sem, lon_send_sem, lon_recv_sem, lat_send_sem, lat_recv_sem,
    ) = rest
    p = lax.axis_index("lat")
    j = lax.axis_index("lon")

    def loop(count, body):
        lax.fori_loop(0, count, lambda i, _: (body(i), 0)[1], 0)

    ens = lax.axis_index("ens")
    lon_ring = [(dx, dy) for dx in (2, 1, 3, 0) for dy in (0, 1)]
    lat_ring = [(dz, dc) for dz in (4, 3, 5, 2, 6, 1, 7, 0) for dc in (0, 1)]

    def lon_peers(sign):
        return [lax.rem(j // 2 + 4 + sign * dx, 4) * 2 + lax.rem(j + dy, 2) for dx, dy in lon_ring]

    def lat_peers(sign):
        return [lax.rem(p // 2 + 8 + sign * dz, 8) * 2 + lax.rem(p + dc, 2) for dz, dc in lat_ring if dz + dc]

    lon_to, lon_from, lat_to, lat_from = lon_peers(1), lon_peers(-1), lat_peers(1), lat_peers(-1)

    def device(axis, to):
        return {"lon": to, "ens": 1 - ens} if axis == "lon" else {"lat": to}

    held_here = (
        state, weight1, bias_1, weight2, bias_2, gain1, shift1, gain2, shift2, fc1, fc1_bias, fc2, fc2_bias, cotangent,
        ahead, fwd, even, odd, inv,
    )
    loads = [pltpu.make_async_copy(a, b, load_sem.at[i + 1]) for i, (a, b) in enumerate(zip(sources, held_here))]
    state_loads = [pltpu.make_async_copy(sources[0].at[s], state.at[s], load_sem.at[s]) for s in range(2)]
    for load in state_loads[:1] + [loads[i] for i in FIRST] + state_loads[1:]:
        load.start()
    barrier = pltpu.get_barrier_semaphore()
    for axis, peers in (("lat", lat_to), ("lon", lon_to)):
        for to in peers:
            pl.semaphore_signal(barrier, inc=1, device_id=device(axis, to), device_id_type=pl.DeviceIdType.MESH)
    for i in MIDDLE + LAST:
        loads[i].start()
    for i in FIRST:
        loads[i].wait()

    def buffers(x, s, axis):
        e = 2 * x + s
        if axis == "lon":
            return lon_send, lon_recv, lon_send_sem, lon_recv_sem, e, j
        return lat_send, lat_recv, lat_send_sem, lat_recv_sem, e, p

    def copy(x, s, axis, to, start, rows, part):
        send, recv, send_sem, recv_sem, e, me = buffers(x, s, axis)
        return pltpu.make_async_remote_copy(
            src_ref=send.at[e, to, pl.ds(start, rows)],
            dst_ref=recv.at[e, me, pl.ds(start, rows)],
            send_sem=send_sem.at[e],
            recv_sem=recv_sem.at[e, part],
            device_id=device(axis, to),
            device_id_type=pl.DeviceIdType.MESH,
        )

    def several(x, s, axis, count, start, rows, part):
        send, recv, send_sem, recv_sem, e, me = buffers(x, s, axis)
        return pltpu.make_async_remote_copy(
            src_ref=send.at[e, pl.ds(0, count), pl.ds(start, rows)],
            dst_ref=recv.at[e, pl.ds(0, count), pl.ds(start, rows)],
            send_sem=send_sem.at[e],
            recv_sem=recv_sem.at[e, part],
            device_id=device(axis, lon_to[0] if axis == "lon" else lat_to[0]),
            device_id_type=pl.DeviceIdType.MESH,
        )

    class sender:
        def __init__(self, x, s, axis):
            self.where = (x, s, axis)

        def __call__(self, to, values, start=0):
            send, recv, _, _, e, _ = buffers(*self.where)
            (recv if to is p else send)[e, to, start : start + values.shape[0]] = values.astype(BF16)

        def send(self, group, start, rows, part):
            for to in group:
                if to is not p:
                    copy(*self.where, to, start, rows, part).start()

    class receiver:
        def __init__(self, x, s, axis):
            self.where = (x, s, axis)

        def wait(self, count, start, rows, part):
            several(*self.where, count, start, rows, part).wait_recv()

        def __call__(self, source, start=0, rows=112):
            _, recv, _, _, e, _ = buffers(*self.where)
            return recv[e, source, start : start + rows]

    lon_tos, lon_froms = [lon_to[:4], lon_to[4:]], [lon_from[:4], lon_from[4:]]
    lat_tos, lat_froms = [lat_to[:8], lat_to[8:] + [p]], [p] + lat_from

    def tokens(ref, s):
        return jnp.concatenate([ref[s, r].astype(F32) for r in range(R)], axis=0)

    def out_tokens(ref, s, values):
        for r in range(R):
            ref[s, r] = values[C * r : C * r + C].astype(BF16)

    def held(s):
        return slice(TOK * s, TOK * s + TOK)

    def send_tokens(x, s, ref):
        e = 2 * x + s
        for b in range(NJ):
            lon_send[e, b] = pack_lon(feature_block(lambda t: ref[s, :, 128 * t : 128 * t + 128], b)).astype(BF16)
        if e == 0:
            pl.semaphore_wait(barrier, NP - 1 + NJ)
        for half in range(2):
            for to in lon_tos[half]:
                copy(x, s, "lon", to, 0, 112, half).start()

    def first_norm(s):
        with jax.named_scope("ln"):
            state_loads[s].wait()
            normed, _ = layer_norm(tokens(state, s))
            lowered[s] = (normed * row(gain1) + row(shift1)).astype(BF16).astype(F32)
            send_tokens(0, s, lowered)

    def cot_product(start, stop):
        with jax.named_scope("gh"):
            cots = jnp.concatenate([tokens(cotangent, s) for s in range(2)], axis=0).astype(BF16)
            for n in range(start, stop):
                cols = slice(n * HC, n * HC + HC)
                gh[:, cols] = dot_nt(cots, fc2[cols, :])

    first_norm(0)
    for i in MIDDLE:
        loads[i].wait()
    fill_matrix(mat1, weight1)
    fill_matrix(mat2, weight2)
    fill_transposed(turned1, mat1)
    fill_transposed(turned2, mat2)
    fill_bias(bias1, bias_1)
    fill_bias(bias2, bias_2)
    fill_first(fwd0, inv0, fwd, inv, p == 0)
    loads[11].wait()
    cot_product(0, 2)
    first_norm(1)
    cot_product(2, 4)

    for s in range(2):
        with jax.named_scope("w0"):
            width_ahead(lon_froms, receiver(0, s, "lon"), wide, tall, ahead, lat_tos, sender(0, s, "lat"))
    cot_product(4, 6)

    for s in range(2):
        get, put = receiver(0, s, "lat"), sender(1, s, "lat")
        for part in range(2):
            with jax.named_scope(f"h0{part}"):
                height_ahead(part, lat_froms, get, eights, fours, spec, fwd, fwd0)
            with jax.named_scope(f"sp0{part}"):
                spectral_ahead(part, spec, first_pre.at[s], squares.at[s], mat1, bias1, mat2, bias2)
            with jax.named_scope(f"hb1{part}"):
                height_back(part, spec, eights, fours, inv, inv0, lat_tos, put)
    for s in range(2):
        with jax.named_scope("slopes"):
            spectral_slopes(first_pre.at[s])
    loads[9].wait()
    for s in range(2):
        with jax.named_scope("wb1"):
            width_back(lat_froms, receiver(1, s, "lat"), tall, wide, even, odd, lon_tos, sender(1, s, "lon"))
    for s in range(2):
        with jax.named_scope("gath1"):
            filtered = gathered(receiver(1, s, "lon"))
            mixed[s] = (filtered + lowered[s] + tokens(state, s)).astype(BF16).astype(F32)
        with jax.named_scope("token"):
            grads[s] = token_ahead(
                loop, mixed[s], tokens(cotangent, s), held(s), fc1, fc1_bias, row(gain2), row(shift2), hidden, gh, acc
            )
        with jax.named_scope("sendt"):
            send_tokens(2, s, grads)

    def store(i, s):
        source, target = ((advanced, advanced_hbm), (sensitivity, sensitivity_hbm))[i]
        return pltpu.make_async_copy(source.at[s], target.at[s], store_sem.at[2 * i + s])

    def advance(s):
        for n in range(D // 256):
            cols = slice(256 * n, 256 * n + 256)
            values = dot(hidden[TOK * s : TOK * s + TOK, :], fc2[:, cols]) + fc2_bias[cols].reshape(1, -1) + mixed[s, :, cols]
            for r in range(R):
                advanced[s, r, :, cols] = values[C * r : C * r + C].astype(BF16)

    for s in range(2):
        with jax.named_scope("w2"):
            width_ahead(lon_froms, receiver(2, s, "lon"), wide, tall, ahead, lat_tos, sender(2, s, "lat"))
    for s in range(2):
        with jax.named_scope("adv"):
            advance(s)
        store(0, s).start()
    for s in range(2):
        get, put = receiver(2, s, "lat"), sender(3, s, "lat")
        for part in range(2):
            with jax.named_scope(f"h2{part}"):
                height_ahead(part, lat_froms, get, eights, fours, spec, fwd, fwd0)
            with jax.named_scope(f"sp2{part}"):
                spectral_adjoint(part, spec, first_pre.at[s], squares.at[s], turned1, turned2)
            with jax.named_scope(f"hb3{part}"):
                height_back(part, spec, eights, fours, inv, inv0, lat_tos, put)
    for s in range(2):
        with jax.named_scope("wb3"):
            width_back(lat_froms, receiver(3, s, "lat"), tall, wide, even, odd, lon_tos, sender(3, s, "lon"))
    for s in range(2):
        with jax.named_scope("final"):
            grad = grads[s]
            grad_lowered = gathered(receiver(3, s, "lon")) + grad
            normed, inverse = layer_norm(tokens(state, s))
            out_tokens(sensitivity, s, grad + norm_backward(grad_lowered, row(gain1), normed, inverse))
        store(1, s).start()
    with jax.named_scope("tail_sent"):
        for x in range(4):
            for s in range(2):
                several(x, s, "lon", NJ, 0, 112, 0).wait_send()
                several(x, s, "lat", NP - 1, 0, 56, 0).wait_send()
    with jax.named_scope("tail_store"):
        for i in range(2):
            for s in range(2):
                store(i, s).wait()


def finish(advanced, sensitivity, advanced_out, sensitivity_out, held, sem):
    pieces = [(i, s, slice(3 * h, 3 * h + 3)) for i in range(2) for s in range(2) for h in range(2)]
    arrays = ((advanced, advanced_out), (sensitivity, sensitivity_out))
    come = [
        pltpu.make_async_copy(arrays[i][0].at[s, r], held.at[i, s, r], sem.at[0, n]) for n, (i, s, r) in enumerate(pieces)
    ]
    leave = [
        pltpu.make_async_copy(held.at[i, s, r], arrays[i][1].at[s, r], sem.at[1, n]) for n, (i, s, r) in enumerate(pieces)
    ]
    for copy in come:
        copy.start()
    for arriving, leaving in zip(come, leave):
        arriving.wait()
        leaving.start()
    for copy in leave:
        copy.wait()


def shards(
    state, spec_weight1, spec_bias1, spec_weight2, spec_bias2, norm1_gain, norm1_bias, norm2_gain, norm2_bias,
    fc1_weight, fc1_bias, fc2_weight, fc2_bias, cotangent,
):
    vmem = pl.BlockSpec(memory_space=pltpu.VMEM)
    hbm = pl.BlockSpec(memory_space=pltpu.HBM)
    names = [jnp.asarray(t) for t in tables()]
    operands = [
        state, spec_weight1, spec_bias1, spec_weight2, spec_bias2, norm1_gain, norm1_bias, norm2_gain,
        norm2_bias, fc1_weight, fc1_bias, fc2_weight, fc2_bias, cotangent, *names,
    ]
    specs = [hbm] * len(operands)
    out = jax.ShapeDtypeStruct(state.shape, BF16)
    results = pl.pallas_call(
        kernel,
        out_shape=(out, out),
        in_specs=specs,
        out_specs=(hbm, hbm),
        scratch_shapes=[
            pltpu.VMEM(state.shape, BF16),
            pltpu.VMEM(state.shape, BF16),
            *[pltpu.VMEM(a.shape, a.dtype) for a in operands],
            pltpu.VMEM((8, NJ, 112, 128), BF16),
            pltpu.VMEM((8, NJ, 112, 128), BF16),
            pltpu.VMEM((8, NP, 56, 128), BF16),
            pltpu.VMEM((8, NP, 56, 128), BF16),
            pltpu.VMEM((2, TOK, D), F32),
            pltpu.VMEM((2, TOK, D), F32),
            pltpu.VMEM((2, TOK, D), F32),
            pltpu.VMEM((2 * TOK, FF), BF16),
            pltpu.VMEM((2 * TOK, FF), F32),
            pltpu.VMEM((TOK, D), F32),
            pltpu.VMEM((W, D), F32),
            pltpu.VMEM((16 * NP, D), F32),
            pltpu.VMEM((8 * H, 128), F32),
            pltpu.VMEM((4 * H, 128), F32),
            pltpu.VMEM((ROWS, 256), F32),
            pltpu.VMEM((2, ROWS, 256), F32),
            pltpu.VMEM((2, ROWS, 256), F32),
            pltpu.VMEM((1, 256, 256), BF16),
            pltpu.VMEM((1, 256, 256), BF16),
            pltpu.VMEM((1, 256, 256), BF16),
            pltpu.VMEM((1, 256, 256), BF16),
            pltpu.VMEM((1, 256), F32),
            pltpu.VMEM((1, 256), F32),
            pltpu.VMEM((2, 4 * H, 2 * H), BF16),
            pltpu.VMEM((2 * H, 4 * H), BF16),
            pltpu.SemaphoreType.DMA((len(operands) + 1,)),
            pltpu.SemaphoreType.DMA((4,)),
            pltpu.SemaphoreType.DMA((8,)),
            pltpu.SemaphoreType.DMA((8, 2)),
            pltpu.SemaphoreType.DMA((8,)),
            pltpu.SemaphoreType.DMA((8, 2)),
        ],
        compiler_params=pltpu.CompilerParams(
            collective_id=0, has_side_effects=True, vmem_limit_bytes=67043328
        ),
        name="block",
    )(*operands)
    return pl.pallas_call(
        finish,
        out_shape=(out, out),
        in_specs=[hbm, hbm],
        out_specs=(hbm, hbm),
        scratch_shapes=[pltpu.VMEM((2, *state.shape), BF16), pltpu.SemaphoreType.DMA((2, 8))],
        compiler_params=pltpu.CompilerParams(vmem_limit_bytes=67043328),
        name="finish",
    )(*results)


def solution(mesh):
    in_specs = (
        P("ens", "lat", "lon", None),
        P(None, "lon", None, None),
        P(None, "lon", None),
        P(None, "lon", None, None),
        P(None, "lon", None),
        P(), P(), P(), P(), P(), P(), P(), P(),
        P("ens", "lat", "lon", None),
    )
    out_specs = (P("ens", "lat", "lon", None), P("ens", "lat", "lon", None))
    return jax.shard_map(shards, mesh=mesh, in_specs=in_specs, out_specs=out_specs, check_vma=False)
```
